256 devices in a mesh: dp: 64 (over z, x_hi, y), mp: 4 (over x_lo, core).
Axes of the slice: x: 4 (x_hi: 2, x_lo: 2; x = x_hi * 2 + x_lo), y: 4, z: 8, core: 2. Of those that a mesh axis runs over, the one named last changes fastest.
Arguments:
- gradients: bfloat16 [64, 1024, 6144], P('dp', None, 'mp'), may hold values from -128 to 128
- weights: bfloat16 [1024, 6144], P(None, 'mp'), may hold values from -3 to 3
- master: float32 [1024, 6144], P('dp', 'mp'), may hold values from -6 to 6
- moment_one: float32 [1024, 6144], P('dp', 'mp'), may hold values from -6 to 6
- moment_two: float32 [1024, 6144], P('dp', 'mp'), may hold values from 0.25 to 4
- group_ids: int32 [1024], replicated, may hold values from 0 to 31, never falling along the last dimension, each value on 1 to 64 neighbouring positions
Outputs:
- new_weights: bfloat16 [1024, 6144], P(None, 'mp')
- new_master: float32 [1024, 6144], P('dp', 'mp')
- new_first: float32 [1024, 6144], P('dp', 'mp')
- new_second: float32 [1024, 6144], P('dp', 'mp')
The draws below stay inside these ranges and needn't reach their ends.
Inputs may be any that keep to these rules, and one draw needn't show every extreme that they name: `group_ids`: group numbers never fall along the rows; each group has 1 to 64 rows and every group is present.
All inputs are finite; a program needn't handle non-finite values.
Results may differ from the reference program's by a relative error of at most 0.001.
The reference program's roundings to bfloat16 on the way count: a program that leaves them out, or rounds other values in their place, can miss the bound.
Values may be sent and summed in bfloat16 or wider, within the bound.
A program may use at most 64 MiB of HBM per device.

```python
import math
import jax
import jax.numpy as jnp
import numpy as np
from jax import lax

D = 6144
MOST = 64
ROWS_ALL = 1024
GROUPS = 32
N_DP = 64


def raised(drawn, own_key, source, target, shards_of, factor):
    def block_of(dim):
        return (jnp.arange(drawn.shape[dim]) // (drawn.shape[dim] // shards_of)).reshape((-1,) + (1,) * (drawn.ndim - 1 - dim))

    first = jax.random.permutation(own_key, shards_of)[block_of(target)]
    other_side = (block_of(target) + shards_of // 2) % shards_of
    return jnp.where((block_of(source) == first) | (block_of(source) == other_side), factor * drawn, drawn)


def level_of(rng, extent, split, low, top_value):
    level = 1.0
    for axis_at, shards_of in split:
        draws = jax.random.uniform(jax.random.fold_in(jax.random.fold_in(rng, 6), axis_at), (shards_of,), jnp.float32, low / len(split), top_value / len(split))
        level = level * jnp.repeat(jnp.exp(draws), extent[axis_at] // shards_of).reshape((-1,) + (1,) * (len(extent) - 1 - axis_at))
    return level


def length_profile(amount, total, limit, slope):
    portions = [(1 << 20) // math.isqrt(grade ** slope) + 1 for grade in range(2, amount + 1)]
    rest, holding = total - limit - (amount - 1), [1] * (amount - 1)
    while rest > 0:
        candidates = [i for i in range(amount - 1) if holding[i] < limit]
        pool, budget = sum([portions[i] for i in candidates]), rest
        for i in candidates:
            more = min(limit - holding[i], max(1, budget * portions[i] // pool), rest)
            holding[i] = holding[i] + more
            rest = rest - more
    return np.array([limit] + holding)


def uneven(rng, number_of, total, most, lean):
    if number_of == 2:
        one = jax.random.randint(rng, (), max(1, total - most), min(most, total - 1) + 1)
        return jnp.stack([one, total - one])
    sizes = jnp.asarray(length_profile(number_of, total, most, lean), jnp.int32)
    pairs = (number_of - 1) // 2
    giver, sink = sizes[1:1 + 2 * pairs:2], sizes[2:2 + 2 * pairs:2]
    slack = jnp.minimum(giver - 1, most - sink)
    moved = jax.random.randint(jax.random.fold_in(rng, 1), (pairs,), 0, 1 << 20) % (slack + 1)
    sizes = sizes.at[1:1 + 2 * pairs:2].set(giver - moved).at[2:2 + 2 * pairs:2].set(sink + moved)
    return sizes[jax.random.permutation(jax.random.fold_in(rng, 2), number_of)]


def normal_values(stream_key, dims, deviation, most, shards=(), held_as=jnp.bfloat16):
    entries = deviation * jax.random.normal(stream_key, dims, jnp.float32)
    if shards:
        entries = entries * level_of(stream_key, dims, shards, -0.22, 0.18)
    return jnp.clip(entries, -most, most).astype(held_as)


def gaussian_with(stream_key, dims, scale, limit, pieces, heavy, kind=jnp.bfloat16):
    entries = scale * jax.random.normal(stream_key, dims, jnp.float32)
    if pieces:
        entries = entries * level_of(stream_key, dims, pieces, -0.22, 0.18)
    return jnp.clip(raised(entries, jax.random.fold_in(stream_key, 3), *heavy), -limit, limit).astype(kind)


def setup_inputs(seed: int = 0) -> dict:
    key_list = jax.random.split(jax.random.key(seed), 7)
    return {
        "gradients": gaussian_with(key_list[0], (N_DP, ROWS_ALL, D), 8.0, 128.0, ((0, 64), (2, 4)), (0, 1, 64, 4.0)),
        "weights": normal_values(key_list[1], (ROWS_ALL, D), 0.5, 3.0, ((1, 4),)),
        "master": normal_values(key_list[2], (ROWS_ALL, D), 1.0, 6.0, ((0, 64), (1, 4)), jnp.float32),
        "moment_one": normal_values(key_list[3], (ROWS_ALL, D), 1.0, 6.0, ((0, 64), (1, 4)), jnp.float32),
        "moment_two": jnp.clip(jnp.exp(math.log(4.0) - 2.7725887 * jax.random.uniform(key_list[4], (ROWS_ALL, D), jnp.float32) ** level_of(key_list[4], (ROWS_ALL, D), ((0, 64), (1, 4)), -0.2, 0.2)), 0.25, 4.0),
        "group_ids": jnp.searchsorted(jnp.cumsum(uneven(key_list[5], GROUPS, ROWS_ALL, MOST, 0)), jnp.arange(ROWS_ALL), side="right").astype(jnp.int32),
    }


beta_one = 0.9
beta_two = 0.999
adam_eps = 1e-06
weight_decay = 0.01
learn_rate = 0.04
step_count = 100

def reference(gradients, weights, master, moment_one, moment_two, group_ids):
    grad_mean = lax.optimization_barrier(jnp.sum(gradients, axis=0, dtype=jnp.float32)) / N_DP
    new_first = beta_one * moment_one + (1.0 - beta_one) * grad_mean
    new_second = beta_two * moment_two + (1.0 - beta_two) * grad_mean * grad_mean
    correct_one = 1.0 - beta_one ** step_count
    correct_two = 1.0 - beta_two ** step_count
    update = new_first / correct_one / (jnp.sqrt(new_second / correct_two) + adam_eps) + weight_decay * master
    member = (group_ids[:, None] == jnp.arange(GROUPS, dtype=jnp.int32)[None, :]).astype(jnp.float32)
    weight_sq = jnp.dot(lax.optimization_barrier(jnp.sum(master * master, axis=1)), member, precision=lax.Precision.HIGHEST)
    update_sq = jnp.dot(lax.optimization_barrier(jnp.sum(update * update, axis=1)), member, precision=lax.Precision.HIGHEST)
    trust_ratio = jnp.sqrt(weight_sq / (update_sq + 1e-06))
    row_ratio = jnp.dot(member, trust_ratio, precision=lax.Precision.HIGHEST)
    step_size = learn_rate * row_ratio[:, None] * update
    new_master = master - step_size
    delta_bf = lax.optimization_barrier((-step_size).astype(jnp.bfloat16))
    new_weights = (weights.astype(jnp.float32) + delta_bf.astype(jnp.float32)).astype(jnp.bfloat16)
    return (new_weights, new_master, new_first, new_second)
```

```python
import functools

import jax
import jax.numpy as jnp
from jax import lax
from jax.experimental import pallas as pl
from jax.experimental.pallas import tpu as pltpu
from jax.sharding import Mesh
from jax.sharding import PartitionSpec as P

MESH = pl.DeviceIdType.MESH
NAMES = ("z", "xh", "y", "xl", "c")
NZ, NX, NY = 8, 2, 4
ROWS, COLS = 16, 1536
CA = 1024
CB = COLS - CA
PA = 896
PC = COLS - PA
AHEAD = 2
N_SEM = 200

beta_one = 0.9
beta_two = 0.999
adam_eps = 1e-06
weight_decay = 0.01
learn_rate = 0.04
step_count = 100
correct_one = 1.0 - beta_one**step_count
correct_two = 1.0 - beta_two**step_count

f32, bf16 = jnp.float32, jnp.bfloat16


def kernel(
    g_hbm, w_ref, ma_ref, m1_ref, m2_ref, ids_ref,
    nw_ref, nm_ref, nf_ref, ns_ref,
    g, d, ra1, ra3, ra2, rl1, rl3, xs, xr, yp, zs, zr,
    b4, bf4, b3, bs2, br2, bs1, br1, bt, by2, bys, byr, bf, bxr,
    gs, ns1, nr1, ns2, nr2, load_sem, send_sem, recv_sem,
):
    z, x, y = lax.axis_index("z"), lax.axis_index("xh"), lax.axis_index("y")
    xl, core = lax.axis_index("xl"), lax.axis_index("c")
    ox = 1 - x

    def zo(k):
        return lax.rem(z + (k + NZ), NZ)

    def yo(k):
        return lax.rem(y + (k + NY), NY)

    me = (z * NX + x) * NY + y

    def owner(k):
        o = lax.rem(me + (k + 64), 64)
        return {"z": lax.div(o, 8), "xh": lax.rem(lax.div(o, 4), 2), "y": lax.rem(o, 4)}

    yu, yd, y2 = {"y": yo(1)}, {"y": yo(-1)}, {"y": yo(2)}
    zu, zd = {"z": zo(1)}, {"z": zo(-1)}
    xp = {"xh": ox}
    mp_peers = [{"c": 1 - core}, {"xl": 1 - xl}, {"xl": 1 - xl, "c": 1 - core}]
    dp_peers = [owner(k) for k in (1, -1, 2, -2, 3, -3, 4, -4)]

    order = [4, 3, -3, 2, -2, 1, -1, 0]
    loads = []
    for k, dz in enumerate(order):
        c = pltpu.make_async_copy(g_hbm.at[zo(dz)], g.at[zo(dz)], load_sem.at[k])
        c.start()
        loads.append(c)

    barrier = pltpu.get_barrier_semaphore()
    peers = [yu, yd, y2, zu, zd, xp] + mp_peers + dp_peers
    for p in peers:
        pl.semaphore_signal(barrier, 1, device_id=p, device_id_type=MESH)
    pl.semaphore_wait(barrier, len(peers))

    sent = []

    def send(src, dst, dev):
        i = len(sent)
        c = pltpu.make_async_remote_copy(
            src, dst, send_sem.at[i], recv_sem.at[i], device_id=dev, device_id_type=MESH
        )
        c.start()
        sent.append(c)
        return c

    a_cols = pl.ds(0, CA)
    b_cols = pl.ds(CA, CB)

    relay_up, relay_down, direct_up, direct_down, forward = {}, {}, {}, {}, {}
    cross, zup, zdown = {}, {}, {}

    def y_send(k):
        zz = zo(order[k])
        relay_up[k] = send(g.at[zz, 0, yo(2), :, a_cols], rl1.at[k], yu)
        relay_down[k] = send(g.at[zz, 1, yo(2), :, a_cols], rl3.at[k], yd)
        direct_up[k] = send(g.at[zz, :, yo(1), :, a_cols], ra1.at[k], yu)
        direct_down[k] = send(g.at[zz, :, yo(-1), :, a_cols], ra3.at[k], yd)

    def y_forward(k):
        relay_up[k].wait_recv()
        up = send(rl1.at[k], ra2.at[k, 0], yu)
        relay_down[k].wait_recv()
        forward[k] = (up, send(rl3.at[k], ra2.at[k, 1], yd))

    def y_sum(k):
        direct_up[k].wait_recv()
        direct_down[k].wait_recv()
        for c in forward[k]:
            c.wait_recv()
        zz = zo(order[k])

        def total(h):
            return (
                (g[zz, h, y, :, 0:CA].astype(f32) + ra1[k, h].astype(f32))
                + (ra3[k, h].astype(f32) + ra2[k, h].astype(f32))
            )

        xs[k] = total(ox)
        cross[k] = send(xs.at[k], xr.at[k], xp)
        yp[k] = total(x)

    def z_step(k):
        dz = order[k]
        cross[k].wait_recv()
        part = yp[k] + xr[k]
        if dz == 4:
            zs[k] = part
            zup[4] = send(zs.at[k, pl.ds(0, 8)], zr.at[k, pl.ds(0, 8)], zu)
            zdown[4] = send(zs.at[k, pl.ds(8, 8)], zr.at[k, pl.ds(8, 8)], zd)
            return
        if dz == 0:
            zup[1].wait_recv()
            zdown[1].wait_recv()
            gs[:, 0:CA] = part + (zr[order.index(1)] + zr[order.index(-1)])
            return
        chain, dev, far = (zup, zu, 1) if dz > 0 else (zdown, zd, -1)
        step = abs(dz)
        chain[step + 1].wait_recv()
        if step == 3:
            rows = slice(0, 8) if dz > 0 else slice(8, 16)
            rest = slice(8, 16) if dz > 0 else slice(0, 8)
            zs[k, rows] = part[rows] + zr[0, rows]
            zs[k, rest] = part[rest]
        else:
            zs[k] = part + zr[order.index(far * (step + 1))]
        chain[step] = send(zs.at[k], zr.at[k], dev)

    zdir = (zu, zd)
    sign = (1, -1)
    b4c, b3c, bfc, b2c, b1c = {}, {}, {}, {}, {}

    def own_b(dz, h):
        return g[zo(dz), h, :, :, CA:COLS].astype(f32)

    def b_raw4():
        for s in (0, 1):
            b4c[s] = send(g.at[zo(4), s, :, :, b_cols], b4.at[s], zdir[s])

    def b_raw3():
        for h_first in (1, 0):
            for s in (0, 1):
                h = h_first if s == 0 else 1 - h_first
                b3c[s, h] = send(g.at[zo(3 * sign[s]), h, :, :, b_cols], b3.at[s, h], zdir[s])

    def b_forward():
        for s in (0, 1):
            b4c[s].wait_recv()
            bfc[s] = send(b4.at[s], bf4.at[s], zdir[s])

    def b_two(first):
        for s in (0, 1):
            h = (1 - s) if first else s
            b3c[s, h].wait_recv()
            v = own_b(2 * sign[s], h) + b3[s, h].astype(f32)
            if not first:
                bfc[s].wait_recv()
                v = v + bf4[s].astype(f32)
            bs2[s, h] = v
            b2c[s, h] = send(bs2.at[s, h], br2.at[s, h], zdir[s])

    def b_one(first):
        for s in (0, 1):
            h = (1 - s) if first else s
            b2c[s, h].wait_recv()
            bs1[s, h] = own_b(sign[s], h) + br2[s, h]
            b1c[s, h] = send(bs1.at[s, h], br1.at[s, h], zdir[s])

    yc = {}

    def b_total():
        for s in (0, 1):
            for h in (0, 1):
                b1c[s, h].wait_recv()
        for h in (0, 1):
            bt[h] = own_b(0, h) + (br1[0, h] + br1[1, h])
        yc["two_up"] = send(bt.at[0, yo(2)], by2.at[0], yu)
        yc["two_down"] = send(bt.at[1, yo(2)], by2.at[1], yd)

    def b_y_one():
        yc["two_up"].wait_recv()
        bys[0, 0] = bt[0, yo(1)] + by2[0]
        bys[0, 1] = bt[1, yo(1)]
        yc["up"] = send(bys.at[0], byr.at[0], yu)
        yc["two_down"].wait_recv()
        bys[1, 0] = bt[0, yo(-1)]
        bys[1, 1] = bt[1, yo(-1)] + by2[1]
        yc["down"] = send(bys.at[1], byr.at[1], yd)

    def b_y_sum():
        yc["up"].wait_recv()
        yc["down"].wait_recv()
        bf[1] = bt[ox, y] + (byr[0, ox] + byr[1, ox])
        yc["x"] = send(bf.at[1], bxr, xp)
        bf[0] = bt[x, y] + (byr[0, x] + byr[1, x])

    def b_final():
        yc["x"].wait_recv()
        gs[:, CA:COLS] = bf[0] + bxr[...]

    slots = {
        1: [b_forward],
        2: [functools.partial(b_two, True)],
        3: [functools.partial(b_two, False)],
        4: [functools.partial(b_one, True)],
        5: [functools.partial(b_one, False)],
        7: [b_total],
        8: [b_y_one],
        9: [b_y_sum],
        10: [b_final],
    }

    loads[0].wait()
    b_raw4()
    y_send(0)
    loads[1].wait()
    loads[2].wait()
    b_raw3()
    y_send(1)
    for k in range(11):
        if 2 <= k + AHEAD < 8:
            if k + AHEAD > 2:
                loads[k + AHEAD].wait()
            y_send(k + AHEAD)
        if k < 8:
            y_forward(k)
        for f in slots.get(k, []):
            f()
        if 0 <= k - 1 < 8:
            y_sum(k - 1)
        if 0 <= k - 2 < 8:
            z_step(k - 2)

    row = lax.broadcasted_iota(jnp.int32, (ROWS, 128), 0)
    lane = lax.broadcasted_iota(jnp.int32, (ROWS, 128), 1)
    ids = jnp.zeros((ROWS, 128), jnp.int32)
    for i in range(ROWS):
        ids = jnp.where(row == i, ids_ref[me * ROWS + i], ids)
    member = (ids == lane).astype(f32)
    master = ma_ref[...]
    mean = gs[...] / 64.0
    new_first = beta_one * m1_ref[...] + (1.0 - beta_one) * mean
    new_second = beta_two * m2_ref[...] + (1.0 - beta_two) * mean * mean
    nf_ref[...] = new_first
    ns_ref[...] = new_second
    update = (
        new_first / correct_one / (jnp.sqrt(new_second / correct_two) + adam_eps)
        + weight_decay * master
    )
    gs[...] = update
    weight_rows = jnp.sum(master * master, axis=1, keepdims=True)
    update_rows = jnp.sum(update * update, axis=1, keepdims=True)
    weight_part = jnp.sum(member * weight_rows, axis=0, keepdims=True)
    update_part = jnp.sum(member * update_rows, axis=0, keepdims=True)
    first = lax.broadcasted_iota(jnp.int32, (8, 128), 0) == 0
    ns1[...] = jnp.where(first, weight_part, update_part)
    c1 = [send(ns1, nr1.at[i], p) for i, p in enumerate(mp_peers)]
    for c in c1:
        c.wait_recv()
    ns2[...] = (ns1[...] + nr1[0]) + (nr1[1] + nr1[2])
    c2 = [send(ns2, nr2.at[i], p) for i, p in enumerate(dp_peers)]
    for c in c2:
        c.wait_recv()
    sums = ns2[...]
    for i in range(len(dp_peers)):
        sums = sums + nr2[i]
    ratio = jnp.sqrt(sums[0:1] / (sums[1:2] + 1e-06))
    row_ratio = jnp.sum(member * ratio, axis=1, keepdims=True)
    step_size = learn_rate * row_ratio * gs[...]
    d[z, x, y] = (-step_size).astype(bf16)
    nm_ref[...] = ma_ref[...] - step_size

    p_cols = pl.ds(0, PA)
    q_cols = pl.ds(PA, PC)
    halves = (pl.ds(0, 512), pl.ds(512, PA - 512))

    def hop(ref, dev):
        return send(ref, ref, dev)

    cy = [hop(d.at[z, x, y, :, q_cols], dev) for dev in (yu, yd, y2)]
    az, ax, ayu, ayd, afw = {}, {}, {}, {}, []
    az[1] = [hop(d.at[z, x, y, :, p_cols], dev) for dev in (zu, zd)]

    def y_out(dz, other):
        h = ox if other else x
        ref = d.at[zo(dz), h, y, :, p_cols]
        ayu[dz, other] = hop(ref, yu)
        ayd[dz, other] = hop(ref, yd)

    def x_out(dz):
        ax[dz] = hop(d.at[zo(dz), x, y, :, p_cols], xp)

    def x_in(*dzs):
        for dz in dzs:
            ax[dz].wait_recv()
            y_out(dz, True)

    def y_relay(dz, other):
        if other:
            ayd[dz, other].wait_recv()
            afw.append(hop(d.at[zo(dz), ox, yo(1), :, p_cols], yd))
        else:
            ayu[dz, other].wait_recv()
            afw.append(hop(d.at[zo(dz), x, yo(-1), :, p_cols], yu))

    def z_in(step):
        for c in az[step]:
            c.wait_recv()
        if step < 3:
            az[step + 1] = [
                hop(d.at[zo(-step), x, y, :, p_cols], zu),
                hop(d.at[zo(step), x, y, :, p_cols], zd),
            ]
        elif step == 3:
            az[4] = [
                hop(d.at[zo(-3), x, y, :, halves[0]], zu),
                hop(d.at[zo(3), x, y, :, halves[1]], zd),
            ]
        for dz in (-step, step) if step < 4 else (4,):
            x_out(dz)
            y_out(dz, False)

    cz = {}

    def q_out(step, other):
        h = ox if other else x
        far = step - 1
        cz[step, other] = {}
        for s, dev in ((0, zu), (1, zd)):
            if step == 4 and s != int(other):
                continue
            cz[step, other][s] = hop(d.at[zo(-far if s == 0 else far), h, :, :, q_cols], dev)

    def q_in(step, other):
        for s, c in cz[step, other].items():
            c.wait_recv()
        if step < 4:
            q_out(step + 1, other)

    x_out(0)
    y_out(0, False)
    for c in cy:
        c.wait_recv()
    q_out(1, False)
    cx = hop(d.at[z, x, :, :, q_cols], xp)
    z_in(1)
    x_in(0)
    y_relay(0, False)
    q_in(1, False)
    cx.wait_recv()
    q_out(1, True)
    z_in(2)
    x_in(1, -1)
    y_relay(1, False)
    y_relay(-1, False)
    q_in(2, False)
    q_in(1, True)
    z_in(3)
    y_relay(0, True)
    x_in(2, -2)
    y_relay(2, False)
    y_relay(-2, False)
    q_in(3, False)
    q_in(2, True)
    z_in(4)
    y_relay(1, True)
    y_relay(-1, True)
    x_in(3, -3)
    y_relay(3, False)
    y_relay(-3, False)
    q_in(3, True)
    x_in(4)
    y_relay(2, True)
    y_relay(-2, True)
    y_relay(4, False)
    y_relay(3, True)
    y_relay(-3, True)
    y_relay(4, True)
    for key, c in ayd.items():
        if not key[1]:
            c.wait_recv()
    for key, c in ayu.items():
        if key[1]:
            c.wait_recv()
    q_in(4, False)
    q_in(4, True)
    for c in afw:
        c.wait_recv()

    def add(i, _):
        zz, h, v = lax.div(i, 8), lax.rem(lax.div(i, 4), 2), lax.rem(i, 4)
        nw_ref[i] = (w_ref[i].astype(f32) + d[zz, h, v].astype(f32)).astype(bf16)
        return 0

    lax.fori_loop(0, 64, add, 0)
    for c in sent:
        c.wait_send()


def on_device(gradients, weights, master, moment_one, moment_two, group_ids):
    vmem = pl.BlockSpec(memory_space=pltpu.VMEM)
    own = jax.ShapeDtypeStruct((ROWS, COLS), f32)
    V = pltpu.VMEM
    scratch = [
        V((NZ, NX, NY, ROWS, COLS), bf16),
        V((NZ, NX, NY, ROWS, COLS), bf16),
        V((8, 2, ROWS, CA), bf16),
        V((8, 2, ROWS, CA), bf16),
        V((8, 2, ROWS, CA), bf16),
        V((8, ROWS, CA), bf16),
        V((8, ROWS, CA), bf16),
        V((8, ROWS, CA), f32),
        V((8, ROWS, CA), f32),
        V((8, ROWS, CA), f32),
        V((8, ROWS, CA), f32),
        V((8, ROWS, CA), f32),
        V((2, NY, ROWS, CB), bf16),
        V((2, NY, ROWS, CB), bf16),
        V((2, 2, NY, ROWS, CB), bf16),
        V((2, 2, NY, ROWS, CB), f32),
        V((2, 2, NY, ROWS, CB), f32),
        V((2, 2, NY, ROWS, CB), f32),
        V((2, 2, NY, ROWS, CB), f32),
        V((2, NY, ROWS, CB), f32),
        V((2, ROWS, CB), f32),
        V((2, 2, ROWS, CB), f32),
        V((2, 2, ROWS, CB), f32),
        V((2, ROWS, CB), f32),
        V((ROWS, CB), f32),
        V((ROWS, COLS), f32),
        V((8, 128), f32),
        V((3, 8, 128), f32),
        V((8, 128), f32),
        V((8, 8, 128), f32),
        pltpu.SemaphoreType.DMA((8,)),
        pltpu.SemaphoreType.DMA((N_SEM,)),
        pltpu.SemaphoreType.DMA((N_SEM,)),
    ]
    new_weights, new_master, new_first, new_second = pl.pallas_call(
        kernel,
        out_shape=(jax.ShapeDtypeStruct((64, ROWS, COLS), bf16), own, own, own),
        in_specs=[pl.BlockSpec(memory_space=pl.ANY), vmem, vmem, vmem, vmem,
                  pl.BlockSpec(memory_space=pltpu.SMEM)],
        out_specs=(vmem, vmem, vmem, vmem),
        scratch_shapes=scratch,
        name="lamb",
        compiler_params=pltpu.CompilerParams(
            collective_id=0, has_side_effects=True, vmem_limit_bytes=48 * 2**20
        ),
    )(
        gradients.reshape(NZ, NX, NY, ROWS, COLS),
        weights.reshape(64, ROWS, COLS),
        master, moment_one, moment_two, group_ids,
    )
    return (new_weights.reshape(1024, COLS), new_master, new_first, new_second)


def solution(mesh):
    torus = Mesh(mesh.devices.reshape(8, 2, 4, 2, 2), NAMES)
    dp, mp = ("z", "xh", "y"), ("xl", "c")
    return jax.shard_map(
        on_device,
        mesh=torus,
        in_specs=(P(dp, None, mp), P(None, mp), P(dp, mp), P(dp, mp), P(dp, mp), P()),
        out_specs=(P(None, mp), P(dp, mp), P(dp, mp), P(dp, mp)),
        check_vma=False,
    )
```

```python
import functools

import jax
import jax.numpy as jnp
from jax import lax
from jax.experimental import pallas as pl
from jax.experimental.pallas import tpu as pltpu
from jax.sharding import Mesh
from jax.sharding import PartitionSpec as P

MESH = pl.DeviceIdType.MESH
NAMES = ("z", "xh", "y", "xl", "c")
NZ, NX, NY = 8, 2, 4
ROWS, COLS = 16, 1536
CA = 1024
CB = COLS - CA
PA = 896
PC = COLS - PA
FAR = ((0, False), (4, True))
N_SEND, N_RECV = 21, 104

beta_one = 0.9
beta_two = 0.999
adam_eps = 1e-06
weight_decay = 0.01
learn_rate = 0.04
step_count = 100
correct_one = 1.0 - beta_one**step_count
correct_two = 1.0 - beta_two**step_count

f32, bf16 = jnp.float32, jnp.bfloat16


def kernel(
    g_hbm, w_hbm, in_ref, nw_ref, own_ref,
    g, d, w,
    ra, rl, xs, xr, yp, zs, zr,
    b4, bf4, b3, bs, br, bt, by2, bys, byr, bf, bxr,
    gs, norm_send, norm_recv, load_sem, send_sem, recv_sem,
):
    z, x, y = lax.axis_index("z"), lax.axis_index("xh"), lax.axis_index("y")
    xl, core = lax.axis_index("xl"), lax.axis_index("c")
    ox = 1 - x

    def zo(k):
        return lax.rem(z + (k + NZ), NZ)

    def yo(k):
        return lax.rem(y + (k + NY), NY)

    me = (z * NX + x) * NY + y

    def owner(k):
        o = lax.rem(me + (k + 64), 64)
        return {"z": lax.div(o, 8), "xh": lax.rem(lax.div(o, 4), 2), "y": lax.rem(o, 4)}

    yu, yd, y2 = {"y": yo(1)}, {"y": yo(-1)}, {"y": yo(2)}
    zu, zd, zu2, zd2 = ({"z": zo(k)} for k in (1, -1, 2, -2))
    xp = {"xh": ox}
    mp_far = ({}, {"c": 1 - core}, {"xl": 1 - xl}, {"xl": 1 - xl, "c": 1 - core})
    norm_peers = []
    for k in (4, -4, 3, -3, 2, -2, 1, -1, 0):
        to = owner(k) if k else {}
        norm_peers += [{**to, **far} for far in mp_far if k or far]

    barrier = pltpu.get_barrier_semaphore()
    cross_peers = [{**xp, **to} for to in (yu, yd, y2)]
    peers = [yu, yd, y2, zu, zd, zu2, zd2, xp] + cross_peers + norm_peers
    for p in peers:
        pl.semaphore_signal(barrier, 1, device_id=p, device_id_type=MESH)

    order = [4, 3, -3, 2, -2, 1, -1, 0]
    loads = []

    def load(src, dst):
        c = pltpu.make_async_copy(src, dst, load_sem.at[len(loads)])
        c.start()
        loads.append(c)

    for dz in order:
        load(g_hbm.at[zo(dz)], g.at[zo(dz)])
    load(w_hbm, w)

    pl.semaphore_wait(barrier, len(peers))

    send_ids, recv_ids = {}, {}

    def send(src, dst, dev, out, into):
        i = send_ids.setdefault(out, len(send_ids))
        j = recv_ids.setdefault(into, len(recv_ids))
        pltpu.make_async_remote_copy(
            src, dst, send_sem.at[i], recv_sem.at[j], device_id=dev, device_id_type=MESH
        ).start()

    def take(ref, sem):
        pltpu.make_async_copy(ref, ref, sem).wait()

    def arrived(ref, *into):
        take(ref, recv_sem.at[recv_ids[into]])

    def gone(ref, *out):
        take(ref, send_sem.at[send_ids[out]])

    a_cols = pl.ds(0, CA)
    b_cols = pl.ds(CA, CB)

    def y_start(k):
        zz = zo(order[k])
        send(g.at[zz, 0, yo(2), :, a_cols], rl.at[k, 0], yu, ("y",), ("rl", k))
        send(g.at[zz, 1, yo(2), :, a_cols], rl.at[k, 1], yd, ("y",), ("rl", k))

    def y_direct(k):
        zz = zo(order[k])
        send(g.at[zz, :, yo(1), :, a_cols], ra.at[k, pl.ds(0, 2)], yu, ("y",), ("ra", k))
        send(g.at[zz, :, yo(-1), :, a_cols], ra.at[k, pl.ds(2, 2)], yd, ("y",), ("ra", k))

    def y_forward(k):
        arrived(rl.at[k], "rl", k)
        send(rl.at[k, 0], ra.at[k, 4], yu, ("y",), ("ra", k))
        send(rl.at[k, 1], ra.at[k, 5], yd, ("y",), ("ra", k))

    def y_sum(k):
        arrived(ra.at[k], "ra", k)
        zz = zo(order[k])

        def total(h):
            return (
                (g[zz, h, y, :, 0:CA].astype(f32) + ra[k, h].astype(f32))
                + (ra[k, 2 + h].astype(f32) + ra[k, 4 + h].astype(f32))
            )

        xs[k] = total(ox)
        send(xs.at[k], xr.at[k], xp, ("x",), ("x", k))
        yp[k] = total(x)

    def z_step(k):
        dz = order[k]
        arrived(xr.at[k], "x", k)
        part = yp[k] + xr[k]
        if dz == 4:
            zs[k] = part
            up, down = pl.ds(0, 8), pl.ds(8, 8)
            send(zs.at[k, up], zr.at[k, up], zu, ("z",), ("z", 4))
            send(zs.at[k, down], zr.at[k, down], zd, ("z",), ("z", -4))
            return
        if dz == 0:
            up, down = order.index(1), order.index(-1)
            arrived(zr.at[up], "z", 1)
            arrived(zr.at[down], "z", -1)
            gs[:, 0:CA] = part + (zr[up] + zr[down])
            return
        step = abs(dz)
        if step == 3:
            rows = slice(0, 8) if dz > 0 else slice(8, 16)
            rest = slice(8, 16) if dz > 0 else slice(0, 8)
            arrived(zr.at[0, pl.ds(0, 8)], "z", 4 if dz > 0 else -4)
            zs[k, rows] = part[rows] + zr[0, rows]
            zs[k, rest] = part[rest]
        else:
            far = dz + 1 if dz > 0 else dz - 1
            arrived(zr.at[order.index(far)], "z", far)
            zs[k] = part + zr[order.index(far)]
        send(zs.at[k], zr.at[k], zu if dz > 0 else zd, ("z",), ("z", dz))

    zdir = (zu, zd)
    sign = (1, -1)

    def own_b(dz, h):
        return g[zo(dz), h, :, :, CA:COLS].astype(f32)

    def b_raw4():
        for s in (0, 1):
            send(g.at[zo(4), s, :, :, b_cols], b4.at[s], zdir[s], ("b",), ("b4",))

    def b_raw3():
        for first in (True, False):
            for s in (0, 1):
                h = (1 - s) if first else s
                src = g.at[zo(3 * sign[s]), h, :, :, b_cols]
                send(src, b3.at[s, h], zdir[s], ("b",), ("b3", first))

    def b_forward():
        arrived(b4, "b4")
        for s in (0, 1):
            send(b4.at[s], bf4.at[s], zdir[s], ("b",), ("bf",))

    def b_two(first):
        arrived(b3.at[0], "b3", first)
        if not first:
            arrived(bf4, "bf")
        for s in (0, 1):
            h = (1 - s) if first else s
            v = own_b(2 * sign[s], h) + b3[s, h].astype(f32)
            if not first:
                v = v + bf4[s].astype(f32)
            bs[0, s, h] = v
            send(bs.at[0, s, h], br.at[0, s, h], zdir[s], ("bs",), ("b2", first))

    def b_one(first):
        arrived(br.at[0, 0], "b2", first)
        for s in (0, 1):
            h = (1 - s) if first else s
            bs[1, s, h] = own_b(sign[s], h) + br[0, s, h]
            send(bs.at[1, s, h], br.at[1, s, h], zdir[s], ("bs",), ("b1",))

    def b_total():
        arrived(br.at[1], "b1")
        for h in (0, 1):
            bt[h] = own_b(0, h) + (br[1, 0, h] + br[1, 1, h])
        send(bt.at[0, yo(2)], by2.at[0], yu, ("by2",), ("by2",))
        send(bt.at[1, yo(2)], by2.at[1], yd, ("by2",), ("by2",))

    def b_y_one():
        arrived(by2, "by2")
        bys[0, 0] = bt[0, yo(1)] + by2[0]
        bys[0, 1] = bt[1, yo(1)]
        send(bys.at[0], byr.at[0], yu, ("by",), ("by",))
        bys[1, 0] = bt[0, yo(-1)]
        bys[1, 1] = bt[1, yo(-1)] + by2[1]
        send(bys.at[1], byr.at[1], yd, ("by",), ("by",))

    def b_y_sum():
        arrived(byr, "by")
        bf[1] = bt[ox, y] + (byr[0, ox] + byr[1, ox])
        send(bf.at[1], bxr, xp, ("bx",), ("bx",))
        bf[0] = bt[x, y] + (byr[0, x] + byr[1, x])

    def b_final():
        arrived(bxr, "bx")
        gs[:, CA:COLS] = bf[0] + bxr[...]

    loads[0].wait()
    y_start(0)
    b_raw4()
    loads[1].wait()
    y_start(1)
    y_direct(0)
    loads[2].wait()
    b_raw3()
    for k in range(8):
        if k + 2 < 8:
            for j in (3, 4) if k == 1 else (k + 3,) if 1 < k < 5 else ():
                loads[j].wait()
            y_start(k + 2)
        for j in ((k,) if k < 2 else (2, 3) if k == 2 else (k + 1,)):
            if j < 8:
                y_forward(j)
        if k + 1 < 8:
            y_direct(k + 1)
        if k == 0:
            b_forward()
        if k == 1:
            b_two(True)
        if k == 2:
            b_two(False)
        if k == 3:
            b_one(True)
        if k == 4:
            b_one(False)
        if k >= 1:
            y_sum(k - 1)
        if k >= 3:
            z_step(k - 3)
        if k == 5:
            b_total()
        if k == 6:
            b_y_one()
    b_y_sum()
    z_step(5)
    y_sum(7)
    z_step(6)
    b_final()
    z_step(7)

    lane = lax.broadcasted_iota(jnp.int32, (ROWS, 128), 1)
    wide = (ROWS, 1024)
    mine = lax.broadcasted_iota(jnp.int32, wide, 1) == (
        lax.broadcasted_iota(jnp.int32, wide, 0) + me * ROWS
    )
    ids = jnp.sum(jnp.where(mine, in_ref[3, 0:1, 0:1024], 0.0), axis=1, keepdims=True)
    member = (ids == lane.astype(f32)).astype(f32)
    master = in_ref[0]
    mean = gs[...] / 64.0
    new_first = beta_one * in_ref[1] + (1.0 - beta_one) * mean
    new_second = beta_two * in_ref[2] + (1.0 - beta_two) * mean * mean
    own_ref[1] = new_first
    own_ref[2] = new_second
    update = (
        new_first / correct_one / (jnp.sqrt(new_second / correct_two) + adam_eps)
        + weight_decay * master
    )
    gs[...] = update
    weight_rows = jnp.sum(master * master, axis=1, keepdims=True)
    update_rows = jnp.sum(update * update, axis=1, keepdims=True)
    weight_part = jnp.sum(member * weight_rows, axis=0, keepdims=True)
    update_part = jnp.sum(member * update_rows, axis=0, keepdims=True)
    first = lax.broadcasted_iota(jnp.int32, (8, 128), 0) == 0
    norm_send[...] = jnp.where(first, weight_part, update_part)
    for i, p in enumerate(norm_peers):
        send(norm_send, norm_recv.at[i], p, ("norm",), ("norm",))
    arrived(norm_recv, "norm")
    sums = norm_send[...] + jnp.sum(norm_recv[...], axis=0)
    ratio = jnp.sqrt(sums[0:1] / (sums[1:2] + 1e-06))
    row_ratio = jnp.sum(member * ratio, axis=1, keepdims=True)
    step_size = learn_rate * row_ratio * gs[...]
    d[z, x, y] = (-step_size).astype(bf16)

    p_cols = pl.ds(0, PA)
    q_cols = pl.ds(PA, PC)
    halves = (pl.ds(0, 512), pl.ds(512, PA - 512))
    p_units = {1: d.at[0, 0, 0, :, p_cols], 2: d.at[0, :, 0, :, p_cols], 4: d.at[0, 0, :, :, p_cols],
               8: d.at[0, :, :, :, p_cols], 16: d.at[pl.ds(0, 2), :, :, :, p_cols],
               32: d.at[pl.ds(0, 4), :, :, :, p_cols]}
    q_units = {1: d.at[0, 0, 0, :, q_cols], 2: d.at[0, :, 0, :, q_cols], 4: d.at[0, 0, :, :, q_cols],
               8: d.at[0, :, :, :, q_cols], 16: d.at[pl.ds(0, 2), :, :, :, q_cols],
               32: d.at[pl.ds(0, 4), :, :, :, q_cols]}
    spans = (32, 16, 8, 4, 2, 1)
    count = {"p": 0, "q": 0}

    def hop(kind, ref, dev, *into, whole=True):
        group = next(i for i in range(6) if count[kind] < sum(spans[: i + 1]))
        send(ref, ref, dev, (kind, group), into)
        count[kind] += whole

    def z_own():
        ref = d.at[z, x, y, :, p_cols]
        for step, up, down in ((1, zu, zd), (2, zu2, zd2)):
            hop("p", ref, up, "az", step)
            hop("p", ref, down, "az", step)

    def y_out(other, *dzs):
        h = ox if other else x
        for dz in dzs:
            ref = d.at[zo(dz), h, y, :, p_cols]
            far = (dz, other) in FAR
            relayed = ("relay", abs(dz), other)
            hop("p", ref, yu, *(("end", dz) if far or other else relayed))
            hop("p", ref, yd, *(("end", dz) if far or not other else relayed))
            if far:
                hop("p", ref, y2, "far", dz)

    def x_out(*dzs):
        for dz in dzs:
            hop("p", d.at[zo(dz), x, y, :, p_cols], xp, "ax", abs(dz))

    def x_in(*dzs):
        arrived(p_units[len(dzs)], "ax", abs(dzs[0]))
        y_out(True, *dzs)

    def y_relay(other, *dzs):
        arrived(p_units[len(dzs)], "relay", abs(dzs[0]), other)
        for dz in dzs:
            if other:
                hop("p", d.at[zo(dz), ox, yo(1), :, p_cols], yd, "end", dz)
            else:
                hop("p", d.at[zo(dz), x, yo(-1), :, p_cols], yu, "end", dz)

    def z_in(step):
        arrived(p_units[1 if step == 4 else 2], "az", step)
        if step == 2:
            hop("p", d.at[zo(-2), x, y, :, p_cols], zu, "az", 3)
            hop("p", d.at[zo(2), x, y, :, p_cols], zd, "az", 3)
            hop("p", d.at[zo(-2), x, y, :, halves[0]], zu2, "az", 4, whole=False)
            hop("p", d.at[zo(2), x, y, :, halves[1]], zd2, "az", 4)
        dzs = (-step, step) if step < 4 else (4,)
        x_out(*dzs)
        y_out(False, *dzs)

    def q_out(step, other, v):
        h = ox if other else x
        far = step - 1
        for s, dev in ((0, zu), (1, zd)):
            if step == 4 and s != int(other):
                continue
            if step == 4:
                into = ("q4",)
            elif step == 3 and s != int(other):
                into = ("q3", 3 if s else -3)
            else:
                into = ("q", step, other, v)
            hop("q", d.at[zo(-far if s == 0 else far), h, yo(v), :, q_cols], dev, *into)

    def q_in(step, other, *vs):
        for v in vs:
            arrived(q_units[1 if step == 3 else 2], "q", step, other, v)
            q_out(step + 1, other, v)

    def plane_out():
        ref = d.at[z, x, y, :, q_cols]
        for v, dev in ((-1, yu), (1, yd), (2, y2)):
            hop("q", ref, dev, "plane", False, v)
        hop("q", ref, xp, "plane", True, 0)
        for v, dev in zip((-1, 1, 2), cross_peers):
            hop("q", ref, dev, "plane", True, v)

    def plane_in(other, *vs):
        for v in vs:
            arrived(q_units[1], "plane", other, v)
            q_out(1, other, v)

    def slab_out(*dzs):
        for dz in dzs:
            arrived(p_units[4], "end", dz)
            if dz in (0, 4):
                arrived(p_units[1], "far", dz)
            if abs(dz) == 3:
                arrived(q_units[4], "q3", dz)
            if dz == 4:
                arrived(q_units[8], "q4")
            zz = zo(dz)

            def add(i, _):
                h, v = lax.div(i, NY), lax.rem(i, NY)
                nw_ref[zz, h, v] = (w[zz, h, v].astype(f32) + d[zz, h, v].astype(f32)).astype(bf16)
                return 0

            lax.fori_loop(0, NX * NY, add, 0)

    z_own()
    q_out(1, False, 0)
    plane_out()
    y_out(False, 0)
    x_out(0)
    own_ref[0] = in_ref[0] - step_size
    q_in(1, False, 0)
    z_in(1)
    plane_in(False, 1, -1)
    plane_in(True, 0)
    z_in(2)
    x_in(0)
    plane_in(False, 2)
    plane_in(True, 1, -1, 2)
    q_in(2, False, 0)
    y_relay(False, -1, 1)
    q_in(1, False, 1, -1)
    z_in(3)
    q_in(1, True, 0)
    x_in(-1, 1)
    q_in(1, False, 2)
    z_in(4)
    q_in(1, True, 1, -1, 2)
    y_relay(False, -2, 2)
    x_in(-2, 2)
    y_relay(True, 0)
    q_in(3, False, 0)
    q_in(2, False, 1, -1)
    q_in(2, True, 0)
    x_in(-3, 3)
    y_relay(False, -3, 3)
    q_in(2, False, 2)
    y_relay(True, -1, 1)
    x_in(4)
    q_in(2, True, 1, -1, 2)
    y_relay(True, -2, 2)
    y_relay(False, 4)
    q_in(3, False, 1, -1)
    q_in(3, True, 0)
    y_relay(True, -3, 3)
    q_in(3, False, 2)
    loads[8].wait()
    slab_out(0, -1, 1)
    q_in(3, True, 1, -1, 2)
    gone(g.at[:, :, :, :, a_cols], "y")
    gone(xs, "x")
    gone(zs.at[pl.ds(0, 7)], "z")
    gone(g.at[pl.ds(0, 4), :, :, :, b_cols], "b")
    gone(bs, "bs")
    gone(by2, "by2")
    gone(bys, "by")
    gone(bxr, "bx")
    gone(norm_recv, "norm")
    slab_out(-2, 2)
    slab_out(-3, 3)
    slab_out(4)
    for i, n in enumerate(spans):
        gone(p_units[n], "p", i)
        gone(q_units[n], "q", i)
    assert count == {"p": 63, "q": 63}
    assert (len(send_ids), len(recv_ids)) == (N_SEND, N_RECV), (len(send_ids), len(recv_ids))


def write_out(nw_ref, own_ref, nw_hbm, nm_hbm, nf_hbm, ns_hbm, sem):
    copies = []
    for i in range(4):
        rows = pl.ds(256 * i, 256)
        copies.append(pltpu.make_async_copy(nw_ref.at[rows], nw_hbm.at[rows], sem.at[i]))
    for i, to in enumerate((nm_hbm, nf_hbm, ns_hbm)):
        copies.append(pltpu.make_async_copy(own_ref.at[i], to, sem.at[4 + i]))
    for c in copies:
        c.start()
    for c in copies:
        c.wait()


def on_device(gradients, weights, master, moment_one, moment_two, group_ids):
    V = pltpu.VMEM
    scratch = [
        V((NZ, NX, NY, ROWS, COLS), bf16),
        V((NZ, NX, NY, ROWS, COLS), bf16),
        V((NZ, NX, NY, ROWS, COLS), bf16),
        V((8, 6, ROWS, CA), bf16),
        V((8, 2, ROWS, CA), bf16),
        V((8, ROWS, CA), f32),
        V((8, ROWS, CA), f32),
        V((8, ROWS, CA), f32),
        V((8, ROWS, CA), f32),
        V((8, ROWS, CA), f32),
        V((2, NY, ROWS, CB), bf16),
        V((2, NY, ROWS, CB), bf16),
        V((2, 2, NY, ROWS, CB), bf16),
        V((2, 2, 2, NY, ROWS, CB), f32),
        V((2, 2, 2, NY, ROWS, CB), f32),
        V((2, NY, ROWS, CB), f32),
        V((2, ROWS, CB), f32),
        V((2, 2, ROWS, CB), f32),
        V((2, 2, ROWS, CB), f32),
        V((2, ROWS, CB), f32),
        V((ROWS, CB), f32),
        V((ROWS, COLS), f32),
        V((8, 128), f32),
        V((35, 8, 128), f32),
        pltpu.SemaphoreType.DMA((9,)),
        pltpu.SemaphoreType.DMA((N_SEND,)),
        pltpu.SemaphoreType.DMA((N_RECV,)),
    ]
    hbm, vmem = pl.BlockSpec(memory_space=pltpu.HBM), pl.BlockSpec(memory_space=pltpu.VMEM)
    ids = jnp.pad(group_ids.astype(f32).reshape(1, 1024), ((0, ROWS - 1), (0, COLS - 1024)))
    inputs = jnp.stack([master, moment_one, moment_two, ids])
    new_weights, own = pl.pallas_call(
        kernel,
        out_shape=(
            jax.ShapeDtypeStruct((NZ, NX, NY, ROWS, COLS), bf16),
            jax.ShapeDtypeStruct((3, ROWS, COLS), f32),
        ),
        in_specs=[hbm, hbm, vmem],
        out_specs=(vmem, vmem),
        scratch_shapes=scratch,
        name="lamb",
        compiler_params=pltpu.CompilerParams(
            collective_id=0, has_side_effects=True, vmem_limit_bytes=48 * 2**20
        ),
    )(
        gradients.reshape(NZ, NX, NY, ROWS, COLS),
        weights.reshape(NZ, NX, NY, ROWS, COLS),
        inputs,
    )
    row_block = jax.ShapeDtypeStruct((ROWS, COLS), f32)
    new_weights, new_master, new_first, new_second = pl.pallas_call(
        write_out,
        out_shape=(jax.ShapeDtypeStruct((1024, COLS), bf16),) + (row_block,) * 3,
        in_specs=[pl.BlockSpec(memory_space=pl.ANY)] * 2,
        out_specs=(hbm,) * 4,
        scratch_shapes=[pltpu.SemaphoreType.DMA((7,))],
        compiler_params=pltpu.CompilerParams(vmem_limit_bytes=2**20),
        name="out",
    )(new_weights.reshape(1024, COLS), own)
    return (new_weights, new_master, new_first, new_second)


def solution(mesh):
    torus = Mesh(mesh.devices.reshape(8, 2, 4, 2, 2), NAMES)
    dp, mp = ("z", "xh", "y"), ("xl", "c")
    return jax.shard_map(
        on_device,
        mesh=torus,
        in_specs=(P(dp, None, mp), P(None, mp), P(dp, mp), P(dp, mp), P(dp, mp), P()),
        out_specs=(P(None, mp), P(dp, mp), P(dp, mp), P(dp, mp)),
        check_vma=False,
    )
```

```python
import functools

import jax
import jax.numpy as jnp
from jax import lax
from jax.experimental import pallas as pl
from jax.experimental.pallas import tpu as pltpu
from jax.sharding import Mesh
from jax.sharding import PartitionSpec as P

MESH = pl.DeviceIdType.MESH
NAMES = ("z", "xh", "y", "xl", "c")
NZ, NX, NY = 8, 2, 4
ROWS, COLS = 16, 1536
CA = 1024
CB = COLS - CA
PA = 896
PC = COLS - PA
FAR = ((0, False), (4, True))
N_SEND, N_RECV = 21, 104

beta_one = 0.9
beta_two = 0.999
adam_eps = 1e-06
weight_decay = 0.01
learn_rate = 0.04
step_count = 100
correct_one = 1.0 - beta_one**step_count
correct_two = 1.0 - beta_two**step_count

f32, bf16 = jnp.float32, jnp.bfloat16


def kernel(
    g_hbm, w_hbm, in_ref, nw_ref, own_ref,
    g, d, w,
    ra, rl, xs, xr, yp, zs, zr,
    b4, bf4, b3, bs, br, bt, by2, bys, byr, bf, bxr,
    gs, norm_send, norm_recv, load_sem, send_sem, recv_sem,
):
    z, x, y = lax.axis_index("z"), lax.axis_index("xh"), lax.axis_index("y")
    xl, core = lax.axis_index("xl"), lax.axis_index("c")
    ox = 1 - x

    def zo(k):
        return lax.rem(z + (k + NZ), NZ)

    def yo(k):
        return lax.rem(y + (k + NY), NY)

    me = (z * NX + x) * NY + y

    def owner(k):
        o = lax.rem(me + (k + 64), 64)
        return {"z": lax.div(o, 8), "xh": lax.rem(lax.div(o, 4), 2), "y": lax.rem(o, 4)}

    yu, yd, y2 = {"y": yo(1)}, {"y": yo(-1)}, {"y": yo(2)}
    zu, zd, zu2, zd2 = ({"z": zo(k)} for k in (1, -1, 2, -2))
    xp = {"xh": ox}
    mp_far = ({}, {"c": 1 - core}, {"xl": 1 - xl}, {"xl": 1 - xl, "c": 1 - core})
    norm_peers = []
    for k in (4, -4, 3, -3, 2, -2, 1, -1, 0):
        to = owner(k) if k else {}
        norm_peers += [{**to, **far} for far in mp_far if k or far]

    barrier = pltpu.get_barrier_semaphore()
    cross_peers = [{**xp, **to} for to in (yu, yd, y2)]
    peers = [yu, yd, zu, zd, xp] + norm_peers[-3:]
    for p in peers:
        pl.semaphore_signal(barrier, 1, device_id=p, device_id_type=MESH)

    order = [4, 3, -3, 2, -2, 1, -1, 0]
    loads = []

    def load(src, dst):
        c = pltpu.make_async_copy(src, dst, load_sem.at[len(loads)])
        c.start()
        loads.append(c)

    for dz in order:
        load(g_hbm.at[zo(dz)], g.at[zo(dz)])
    load(w_hbm, w)

    pl.semaphore_wait(barrier, len(peers))

    send_ids, recv_ids = {}, {}

    def send(src, dst, dev, out, into):
        i = send_ids.setdefault(out, len(send_ids))
        j = recv_ids.setdefault(into, len(recv_ids))
        pltpu.make_async_remote_copy(
            src, dst, send_sem.at[i], recv_sem.at[j], device_id=dev, device_id_type=MESH
        ).start()

    def take(ref, sem):
        pltpu.make_async_copy(ref, ref, sem).wait()

    def arrived(ref, *into):
        take(ref, recv_sem.at[recv_ids[into]])

    def gone(ref, *out):
        take(ref, send_sem.at[send_ids[out]])

    a_cols = pl.ds(0, CA)
    b_cols = pl.ds(CA, CB)

    def y_start(k):
        zz = zo(order[k])
        send(g.at[zz, 0, yo(2), :, a_cols], rl.at[k, 0], yu, ("y",), ("rl", k))
        send(g.at[zz, 1, yo(2), :, a_cols], rl.at[k, 1], yd, ("y",), ("rl", k))

    def y_direct(k):
        zz = zo(order[k])
        send(g.at[zz, :, yo(1), :, a_cols], ra.at[k, pl.ds(0, 2)], yu, ("y",), ("ra", k))
        send(g.at[zz, :, yo(-1), :, a_cols], ra.at[k, pl.ds(2, 2)], yd, ("y",), ("ra", k))

    def y_forward(k):
        arrived(rl.at[k], "rl", k)
        send(rl.at[k, 0], ra.at[k, 4], yu, ("y",), ("ra", k))
        send(rl.at[k, 1], ra.at[k, 5], yd, ("y",), ("ra", k))

    def y_sum(k):
        arrived(ra.at[k], "ra", k)
        zz = zo(order[k])

        def total(h):
            return (
                (g[zz, h, y, :, 0:CA].astype(f32) + ra[k, h].astype(f32))
                + (ra[k, 2 + h].astype(f32) + ra[k, 4 + h].astype(f32))
            )

        xs[k] = total(ox)
        send(xs.at[k], xr.at[k], xp, ("x",), ("x", k))
        yp[k] = total(x)

    def z_step(k):
        dz = order[k]
        arrived(xr.at[k], "x", k)
        part = yp[k] + xr[k]
        if dz == 4:
            zs[k] = part
            up, down = pl.ds(0, 8), pl.ds(8, 8)
            send(zs.at[k, up], zr.at[k, up], zu, ("z",), ("z", 4))
            send(zs.at[k, down], zr.at[k, down], zd, ("z",), ("z", -4))
            return
        if dz == 0:
            up, down = order.index(1), order.index(-1)
            arrived(zr.at[up], "z", 1)
            arrived(zr.at[down], "z", -1)
            gs[:, 0:CA] = part + (zr[up] + zr[down])
            return
        step = abs(dz)
        if step == 3:
            rows = slice(0, 8) if dz > 0 else slice(8, 16)
            rest = slice(8, 16) if dz > 0 else slice(0, 8)
            arrived(zr.at[0, pl.ds(0, 8)], "z", 4 if dz > 0 else -4)
            zs[k, rows] = part[rows] + zr[0, rows]
            zs[k, rest] = part[rest]
        else:
            far = dz + 1 if dz > 0 else dz - 1
            arrived(zr.at[order.index(far)], "z", far)
            zs[k] = part + zr[order.index(far)]
        send(zs.at[k], zr.at[k], zu if dz > 0 else zd, ("z",), ("z", dz))

    zdir = (zu, zd)
    sign = (1, -1)

    def own_b(dz, h):
        return g[zo(dz), h, :, :, CA:COLS].astype(f32)

    def b_raw4():
        for s in (0, 1):
            send(g.at[zo(4), s, :, :, b_cols], b4.at[s], zdir[s], ("b",), ("b4",))

    def b_raw3():
        for first in (True, False):
            for s in (0, 1):
                h = (1 - s) if first else s
                src = g.at[zo(3 * sign[s]), h, :, :, b_cols]
                send(src, b3.at[s, h], zdir[s], ("b",), ("b3", first))

    def b_forward():
        arrived(b4, "b4")
        for s in (0, 1):
            send(b4.at[s], bf4.at[s], zdir[s], ("b",), ("bf",))

    def b_two(first):
        arrived(b3.at[0], "b3", first)
        if not first:
            arrived(bf4, "bf")
        for s in (0, 1):
            h = (1 - s) if first else s
            v = own_b(2 * sign[s], h) + b3[s, h].astype(f32)
            if not first:
                v = v + bf4[s].astype(f32)
            bs[0, s, h] = v
            send(bs.at[0, s, h], br.at[0, s, h], zdir[s], ("bs",), ("b2", first))

    def b_one(first):
        arrived(br.at[0, 0], "b2", first)
        for s in (0, 1):
            h = (1 - s) if first else s
            bs[1, s, h] = own_b(sign[s], h) + br[0, s, h]
            send(bs.at[1, s, h], br.at[1, s, h], zdir[s], ("bs",), ("b1",))

    def b_total():
        arrived(br.at[1], "b1")
        for h in (0, 1):
            bt[h] = own_b(0, h) + (br[1, 0, h] + br[1, 1, h])
        send(bt.at[0, yo(2)], by2.at[0], yu, ("by2",), ("by2",))
        send(bt.at[1, yo(2)], by2.at[1], yd, ("by2",), ("by2",))

    def b_y_one():
        arrived(by2, "by2")
        bys[0, 0] = bt[0, yo(1)] + by2[0]
        bys[0, 1] = bt[1, yo(1)]
        send(bys.at[0], byr.at[0], yu, ("by",), ("by",))
        bys[1, 0] = bt[0, yo(-1)]
        bys[1, 1] = bt[1, yo(-1)] + by2[1]
        send(bys.at[1], byr.at[1], yd, ("by",), ("by",))

    def b_y_sum():
        arrived(byr, "by")
        bf[1] = bt[ox, y] + (byr[0, ox] + byr[1, ox])
        send(bf.at[1], bxr, xp, ("bx",), ("bx",))
        bf[0] = bt[x, y] + (byr[0, x] + byr[1, x])

    def b_final():
        arrived(bxr, "bx")
        gs[:, CA:COLS] = bf[0] + bxr[...]

    loads[0].wait()
    y_start(0)
    b_raw4()
    loads[1].wait()
    y_start(1)
    y_direct(0)
    loads[2].wait()
    b_raw3()
    for k in range(8):
        if k + 2 < 8:
            for j in (3, 4) if k == 1 else (k + 3,) if 1 < k < 5 else ():
                loads[j].wait()
            y_start(k + 2)
        for j in ((k,) if k < 2 else (2, 3) if k == 2 else (k + 1,)):
            if j < 8:
                y_forward(j)
        if k + 1 < 8:
            y_direct(k + 1)
        if k == 0:
            b_forward()
        if k == 1:
            b_two(True)
        if k == 2:
            b_two(False)
        if k == 3:
            b_one(True)
        if k == 4:
            b_one(False)
        if k >= 1:
            y_sum(k - 1)
        if k >= 3:
            z_step(k - 3)
        if k == 5:
            b_total()
        if k == 6:
            b_y_one()
    b_y_sum()
    z_step(5)
    y_sum(7)
    z_step(6)
    b_final()
    z_step(7)

    lane = lax.broadcasted_iota(jnp.int32, (ROWS, 128), 1)
    wide = (ROWS, 1024)
    mine = lax.broadcasted_iota(jnp.int32, wide, 1) == (
        lax.broadcasted_iota(jnp.int32, wide, 0) + me * ROWS
    )
    ids = jnp.sum(jnp.where(mine, in_ref[3, 0:1, 0:1024], 0.0), axis=1, keepdims=True)
    member = (ids == lane.astype(f32)).astype(f32)
    master = in_ref[0]
    mean = gs[...] / 64.0
    new_first = beta_one * in_ref[1] + (1.0 - beta_one) * mean
    new_second = beta_two * in_ref[2] + (1.0 - beta_two) * mean * mean
    own_ref[1] = new_first
    own_ref[2] = new_second
    update = (
        new_first / correct_one / (jnp.sqrt(new_second / correct_two) + adam_eps)
        + weight_decay * master
    )
    gs[...] = update
    weight_rows = jnp.sum(master * master, axis=1, keepdims=True)
    update_rows = jnp.sum(update * update, axis=1, keepdims=True)
    weight_part = jnp.sum(member * weight_rows, axis=0, keepdims=True)
    update_part = jnp.sum(member * update_rows, axis=0, keepdims=True)
    first = lax.broadcasted_iota(jnp.int32, (8, 128), 0) == 0
    norm_send[...] = jnp.where(first, weight_part, update_part)
    for i, p in enumerate(norm_peers):
        send(norm_send, norm_recv.at[i], p, ("norm",), ("norm",))
    arrived(norm_recv, "norm")
    sums = norm_send[...] + jnp.sum(norm_recv[...], axis=0)
    ratio = jnp.sqrt(sums[0:1] / (sums[1:2] + 1e-06))
    row_ratio = jnp.sum(member * ratio, axis=1, keepdims=True)
    step_size = learn_rate * row_ratio * gs[...]
    d[z, x, y] = (-step_size).astype(bf16)

    p_cols = pl.ds(0, PA)
    q_cols = pl.ds(PA, PC)
    halves = (pl.ds(0, 512), pl.ds(512, PA - 512))
    p_units = {1: d.at[0, 0, 0, :, p_cols], 2: d.at[0, :, 0, :, p_cols], 4: d.at[0, 0, :, :, p_cols],
               8: d.at[0, :, :, :, p_cols], 16: d.at[pl.ds(0, 2), :, :, :, p_cols],
               32: d.at[pl.ds(0, 4), :, :, :, p_cols]}
    q_units = {1: d.at[0, 0, 0, :, q_cols], 2: d.at[0, :, 0, :, q_cols], 4: d.at[0, 0, :, :, q_cols],
               8: d.at[0, :, :, :, q_cols], 16: d.at[pl.ds(0, 2), :, :, :, q_cols],
               32: d.at[pl.ds(0, 4), :, :, :, q_cols]}
    spans = (32, 16, 8, 4, 2, 1)
    count = {"p": 0, "q": 0}

    def hop(kind, ref, dev, *into, whole=True):
        group = next(i for i in range(6) if count[kind] < sum(spans[: i + 1]))
        send(ref, ref, dev, (kind, group), into)
        count[kind] += whole

    def z_own():
        ref = d.at[z, x, y, :, p_cols]
        for step, up, down in ((1, zu, zd), (2, zu2, zd2)):
            hop("p", ref, up, "az", step)
            hop("p", ref, down, "az", step)

    def y_out(other, *dzs):
        h = ox if other else x
        for dz in dzs:
            ref = d.at[zo(dz), h, y, :, p_cols]
            far = (dz, other) in FAR
            relayed = ("relay", abs(dz), other)
            hop("p", ref, yu, *(("end", dz) if far or other else relayed))
            hop("p", ref, yd, *(("end", dz) if far or not other else relayed))
            if far:
                hop("p", ref, y2, "far", dz)

    def x_out(*dzs):
        for dz in dzs:
            hop("p", d.at[zo(dz), x, y, :, p_cols], xp, "ax", abs(dz))

    def x_in(*dzs):
        arrived(p_units[len(dzs)], "ax", abs(dzs[0]))
        y_out(True, *dzs)

    def y_relay(other, *dzs):
        arrived(p_units[len(dzs)], "relay", abs(dzs[0]), other)
        for dz in dzs:
            if other:
                hop("p", d.at[zo(dz), ox, yo(1), :, p_cols], yd, "end", dz)
            else:
                hop("p", d.at[zo(dz), x, yo(-1), :, p_cols], yu, "end", dz)

    def z_in(step):
        arrived(p_units[1 if step == 4 else 2], "az", step)
        if step == 2:
            hop("p", d.at[zo(-2), x, y, :, p_cols], zu, "az", 3)
            hop("p", d.at[zo(2), x, y, :, p_cols], zd, "az", 3)
            hop("p", d.at[zo(-2), x, y, :, halves[0]], zu2, "az", 4, whole=False)
            hop("p", d.at[zo(2), x, y, :, halves[1]], zd2, "az", 4)
        dzs = (-step, step) if step < 4 else (4,)
        x_out(*dzs)
        y_out(False, *dzs)

    def q_out(step, other, v):
        h = ox if other else x
        far = step - 1
        for s, dev in ((0, zu), (1, zd)):
            if step == 4 and s != int(other):
                continue
            if step == 4:
                into = ("q4",)
            elif step == 3 and s != int(other):
                into = ("q3", 3 if s else -3)
            else:
                into = ("q", step, other, v)
            hop("q", d.at[zo(-far if s == 0 else far), h, yo(v), :, q_cols], dev, *into)

    def q_in(step, other, *vs):
        for v in vs:
            arrived(q_units[1 if step == 3 else 2], "q", step, other, v)
            q_out(step + 1, other, v)

    def plane_out():
        ref = d.at[z, x, y, :, q_cols]
        for v, dev in ((-1, yu), (1, yd), (2, y2)):
            hop("q", ref, dev, "plane", False, v)
        hop("q", ref, xp, "plane", True, 0)
        for v, dev in zip((-1, 1, 2), cross_peers):
            hop("q", ref, dev, "plane", True, v)

    def plane_in(other, *vs):
        for v in vs:
            arrived(q_units[1], "plane", other, v)
            q_out(1, other, v)

    def slab_out(*dzs):
        for dz in dzs:
            arrived(p_units[4], "end", dz)
            if dz in (0, 4):
                arrived(p_units[1], "far", dz)
            if abs(dz) == 3:
                arrived(q_units[4], "q3", dz)
            if dz == 4:
                arrived(q_units[8], "q4")
            zz = zo(dz)

            def add(i, _):
                h, v = lax.div(i, NY), lax.rem(i, NY)
                nw_ref[zz, h, v] = (w[zz, h, v].astype(f32) + d[zz, h, v].astype(f32)).astype(bf16)
                return 0

            lax.fori_loop(0, NX * NY, add, 0)

    z_own()
    q_out(1, False, 0)
    plane_out()
    y_out(False, 0)
    x_out(0)
    own_ref[0] = in_ref[0] - step_size
    q_in(1, False, 0)
    z_in(1)
    plane_in(False, 1, -1)
    plane_in(True, 0)
    z_in(2)
    x_in(0)
    plane_in(False, 2)
    plane_in(True, 1, -1, 2)
    q_in(2, False, 0)
    y_relay(False, -1, 1)
    q_in(1, False, 1, -1)
    z_in(3)
    q_in(1, True, 0)
    x_in(-1, 1)
    q_in(1, False, 2)
    z_in(4)
    q_in(1, True, 1, -1, 2)
    y_relay(False, -2, 2)
    x_in(-2, 2)
    y_relay(True, 0)
    q_in(3, False, 0)
    q_in(2, False, 1, -1)
    q_in(2, True, 0)
    x_in(-3, 3)
    y_relay(False, -3, 3)
    q_in(2, False, 2)
    y_relay(True, -1, 1)
    x_in(4)
    q_in(2, True, 1, -1, 2)
    y_relay(True, -2, 2)
    y_relay(False, 4)
    q_in(3, False, 1, -1)
    q_in(3, True, 0)
    y_relay(True, -3, 3)
    q_in(3, False, 2)
    loads[8].wait()
    slab_out(0, -1, 1)
    q_in(3, True, 1, -1, 2)
    gone(g.at[:, :, :, :, a_cols], "y")
    gone(xs, "x")
    gone(zs.at[pl.ds(0, 7)], "z")
    gone(g.at[pl.ds(0, 4), :, :, :, b_cols], "b")
    gone(bs, "bs")
    gone(by2, "by2")
    gone(bys, "by")
    gone(bxr, "bx")
    gone(norm_recv, "norm")
    slab_out(-2, 2)
    slab_out(-3, 3)
    slab_out(4)
    for i, n in enumerate(spans):
        gone(p_units[n], "p", i)
        gone(q_units[n], "q", i)
    assert count == {"p": 63, "q": 63}
    assert (len(send_ids), len(recv_ids)) == (N_SEND, N_RECV), (len(send_ids), len(recv_ids))


def write_out(nw_ref, own_ref, nw_hbm, nm_hbm, nf_hbm, ns_hbm, sem):
    copies = []
    for i in range(4):
        rows = pl.ds(256 * i, 256)
        copies.append(pltpu.make_async_copy(nw_ref.at[rows], nw_hbm.at[rows], sem.at[i]))
    for i, to in enumerate((nm_hbm, nf_hbm, ns_hbm)):
        copies.append(pltpu.make_async_copy(own_ref.at[i], to, sem.at[4 + i]))
    for c in copies:
        c.start()
    for c in copies:
        c.wait()


def on_device(gradients, weights, master, moment_one, moment_two, group_ids):
    V = pltpu.VMEM
    scratch = [
        V((NZ, NX, NY, ROWS, COLS), bf16),
        V((NZ, NX, NY, ROWS, COLS), bf16),
        V((NZ, NX, NY, ROWS, COLS), bf16),
        V((8, 6, ROWS, CA), bf16),
        V((8, 2, ROWS, CA), bf16),
        V((8, ROWS, CA), f32),
        V((8, ROWS, CA), f32),
        V((8, ROWS, CA), f32),
        V((8, ROWS, CA), f32),
        V((8, ROWS, CA), f32),
        V((2, NY, ROWS, CB), bf16),
        V((2, NY, ROWS, CB), bf16),
        V((2, 2, NY, ROWS, CB), bf16),
        V((2, 2, 2, NY, ROWS, CB), f32),
        V((2, 2, 2, NY, ROWS, CB), f32),
        V((2, NY, ROWS, CB), f32),
        V((2, ROWS, CB), f32),
        V((2, 2, ROWS, CB), f32),
        V((2, 2, ROWS, CB), f32),
        V((2, ROWS, CB), f32),
        V((ROWS, CB), f32),
        V((ROWS, COLS), f32),
        V((8, 128), f32),
        V((35, 8, 128), f32),
        pltpu.SemaphoreType.DMA((9,)),
        pltpu.SemaphoreType.DMA((N_SEND,)),
        pltpu.SemaphoreType.DMA((N_RECV,)),
    ]
    hbm, vmem = pl.BlockSpec(memory_space=pltpu.HBM), pl.BlockSpec(memory_space=pltpu.VMEM)
    ids = jnp.pad(group_ids.astype(f32).reshape(1, 1024), ((0, ROWS - 1), (0, COLS - 1024)))
    inputs = jnp.stack([master, moment_one, moment_two, ids])
    new_weights, own = pl.pallas_call(
        kernel,
        out_shape=(
            jax.ShapeDtypeStruct((NZ, NX, NY, ROWS, COLS), bf16),
            jax.ShapeDtypeStruct((3, ROWS, COLS), f32),
        ),
        in_specs=[hbm, hbm, vmem],
        out_specs=(vmem, vmem),
        scratch_shapes=scratch,
        name="lamb",
        compiler_params=pltpu.CompilerParams(
            collective_id=0, has_side_effects=True, vmem_limit_bytes=48 * 2**20
        ),
    )(
        gradients.reshape(NZ, NX, NY, ROWS, COLS),
        weights.reshape(NZ, NX, NY, ROWS, COLS),
        inputs,
    )
    row_block = jax.ShapeDtypeStruct((ROWS, COLS), f32)
    new_weights, new_master, new_first, new_second = pl.pallas_call(
        write_out,
        out_shape=(jax.ShapeDtypeStruct((1024, COLS), bf16),) + (row_block,) * 3,
        in_specs=[pl.BlockSpec(memory_space=pl.ANY)] * 2,
        out_specs=(hbm,) * 4,
        scratch_shapes=[pltpu.SemaphoreType.DMA((7,))],
        compiler_params=pltpu.CompilerParams(vmem_limit_bytes=2**20),
        name="out",
    )(new_weights.reshape(1024, COLS), own)
    return (new_weights, new_master, new_first, new_second)


def solution(mesh):
    torus = Mesh(mesh.devices.reshape(8, 2, 4, 2, 2), NAMES)
    dp, mp = ("z", "xh", "y"), ("xl", "c")
    return jax.shard_map(
        on_device,
        mesh=torus,
        in_specs=(P(dp, None, mp), P(None, mp), P(dp, mp), P(dp, mp), P(dp, mp), P()),
        out_specs=(P(None, mp), P(dp, mp), P(dp, mp), P(dp, mp)),
        check_vma=False,
    )
```

```python
import functools

import jax
import jax.numpy as jnp
from jax import lax
from jax.experimental import pallas as pl
from jax.experimental.pallas import tpu as pltpu
from jax.sharding import Mesh
from jax.sharding import PartitionSpec as P

MESH = pl.DeviceIdType.MESH
NAMES = ("z", "xh", "y", "xl", "c")
NZ, NX, NY = 8, 2, 4
ROWS, COLS = 16, 1536
CA = 896
CB = 384
CC = COLS - CA - CB
PA = 896
PC = COLS - PA
FAR = ((0, False), (4, True))
N_SEND, N_RECV = 24, 118

beta_one = 0.9
beta_two = 0.999
adam_eps = 1e-06
weight_decay = 0.01
learn_rate = 0.04
step_count = 100
correct_one = 1.0 - beta_one**step_count
correct_two = 1.0 - beta_two**step_count

f32, bf16 = jnp.float32, jnp.bfloat16


def kernel(
    g_hbm, w_hbm, in_ref, nw_ref, own_ref,
    g, d, w,
    ra, rl, xs, xr, yp, zs, zr,
    b4, bf4, b3, bs, br, bt, near_a, near_b, bf, bxr,
    cx, cs, cr, ct, cn,
    gs, norm_send, norm_recv, load_sem, send_sem, recv_sem,
):
    z, x, y = lax.axis_index("z"), lax.axis_index("xh"), lax.axis_index("y")
    xl, core = lax.axis_index("xl"), lax.axis_index("c")
    ox = 1 - x

    def zo(k):
        return lax.rem(z + (k + NZ), NZ)

    def yo(k):
        return lax.rem(y + (k + NY), NY)

    me = (z * NX + x) * NY + y

    def owner(k):
        o = lax.rem(me + (k + 64), 64)
        return {"z": lax.div(o, 8), "xh": lax.rem(lax.div(o, 4), 2), "y": lax.rem(o, 4)}

    yu, yd, y2 = {"y": yo(1)}, {"y": yo(-1)}, {"y": yo(2)}
    zu, zd, zu2, zd2 = ({"z": zo(k)} for k in (1, -1, 2, -2))
    xp = {"xh": ox}
    mp_far = ({}, {"c": 1 - core}, {"xl": 1 - xl}, {"xl": 1 - xl, "c": 1 - core})
    norm_peers = []
    for k in (4, -4, 3, -3, 2, -2, 1, -1, 0):
        to = owner(k) if k else {}
        norm_peers += [{**to, **far} for far in mp_far if k or far]

    barrier = pltpu.get_barrier_semaphore()
    cross_peers = [{**xp, **to} for to in (yu, yd, y2)]
    peers = [yu, yd, zu, zd, xp] + cross_peers + norm_peers[-3:]
    for p in peers:
        pl.semaphore_signal(barrier, 1, device_id=p, device_id_type=MESH)

    order = [4, 3, -3, 2, -2, 1, -1, 0]
    loads = []

    def load(src, dst):
        c = pltpu.make_async_copy(src, dst, load_sem.at[len(loads)])
        c.start()
        loads.append(c)

    for dz in order:
        load(g_hbm.at[zo(dz)], g.at[zo(dz)])
    load(w_hbm, w)

    pl.semaphore_wait(barrier, len(peers))

    send_ids, recv_ids = {}, {}

    def send(src, dst, dev, out, into):
        i = send_ids.setdefault(out, len(send_ids))
        j = recv_ids.setdefault(into, len(recv_ids))
        pltpu.make_async_remote_copy(
            src, dst, send_sem.at[i], recv_sem.at[j], device_id=dev, device_id_type=MESH
        ).start()

    def take(ref, sem):
        pltpu.make_async_copy(ref, ref, sem).wait()

    def arrived(ref, *into):
        take(ref, recv_sem.at[recv_ids[into]])

    def gone(ref, *out):
        take(ref, send_sem.at[send_ids[out]])

    plane = [(False, v, dev) for v, dev in ((1, yu), (-1, yd), (2, y2))]
    plane += [(True, 0, xp)]
    plane += [(True, v, dev) for v, dev in zip((1, -1, 2), cross_peers)]

    a_cols = pl.ds(0, CA)
    b_cols = pl.ds(CA, CB)
    c_cols = pl.ds(CA + CB, CC)

    def y_start(k):
        zz = zo(order[k])
        send(g.at[zz, 0, yo(2), :, a_cols], rl.at[k, 0], yu, ("y",), ("rl", k))
        send(g.at[zz, 1, yo(2), :, a_cols], rl.at[k, 1], yd, ("y",), ("rl", k))

    def y_direct(k):
        zz = zo(order[k])
        send(g.at[zz, :, yo(1), :, a_cols], ra.at[k, pl.ds(0, 2)], yu, ("y",), ("ra", k))
        send(g.at[zz, :, yo(-1), :, a_cols], ra.at[k, pl.ds(2, 2)], yd, ("y",), ("ra", k))

    def y_forward(k):
        arrived(rl.at[k], "rl", k)
        send(rl.at[k, 0], ra.at[k, 4], yu, ("y",), ("ra", k))
        send(rl.at[k, 1], ra.at[k, 5], yd, ("y",), ("ra", k))

    def y_sum(k):
        arrived(ra.at[k], "ra", k)
        zz = zo(order[k])

        def total(h):
            return (
                (g[zz, h, y, :, 0:CA].astype(f32) + ra[k, h].astype(f32))
                + (ra[k, 2 + h].astype(f32) + ra[k, 4 + h].astype(f32))
            )

        xs[k] = total(ox)
        send(xs.at[k], xr.at[k], xp, ("x",), ("x", k))
        yp[k] = total(x)

    def ring(k, part, out, into, tag):
        dz = order[k]
        n = out.shape[1] // 2
        low, high = pl.ds(0, n), pl.ds(n, n)
        if dz == 4:
            out[k] = part
            send(out.at[k, low], into.at[k, low], zu, (tag,), (tag, 4))
            send(out.at[k, high], into.at[k, high], zd, (tag,), (tag, -4))
            return None
        if dz == 0:
            up, down = order.index(1), order.index(-1)
            arrived(into.at[up], tag, 1)
            arrived(into.at[down], tag, -1)
            return part + (into[up] + into[down])
        if abs(dz) == 3:
            rows, rest = slice(0, n), slice(n, 2 * n)
            if dz < 0:
                rows, rest = rest, rows
            arrived(into.at[0, low], tag, 4 if dz > 0 else -4)
            out[k, rows] = part[rows] + into[0, rows]
            out[k, rest] = part[rest]
        else:
            far = dz + 1 if dz > 0 else dz - 1
            arrived(into.at[order.index(far)], tag, far)
            out[k] = part + into[order.index(far)]
        send(out.at[k], into.at[k], zu if dz > 0 else zd, (tag,), (tag, dz))
        return None

    def z_step(k):
        arrived(xr.at[k], "x", k)
        ring(k, yp[k] + xr[k], zs, zr, "z")

    def near_out(across):
        for i, (other, v, dev) in enumerate(plane):
            if other != across:
                continue
            src = g.at[z, ox if other else x, yo(v), :, a_cols]
            send(src, near_a.at[i], dev, ("near_a",), ("near_a",))

    def near_in():
        arrived(near_a, "near_a")
        part = g[z, x, y, :, 0:CA].astype(f32)
        for i in range(len(plane)):
            part = part + near_a[i].astype(f32)
        gs[:, 0:CA] = ring(7, part, zs, zr, "z")

    def c_raw(*ks):
        for k in ks:
            send(g.at[zo(order[k]), ox, :, :, c_cols], cx.at[k], xp, ("cx",), ("cx", k))

    def c_part(k):
        arrived(cx.at[k], "cx", k)
        return g[zo(order[k]), x, :, :, CA + CB : COLS].astype(f32) + cx[k].astype(f32)

    def c_step(*ks):
        for k in ks:
            ring(k, c_part(k), cs, cr, "cz")

    def c_total():
        ct[...] = ring(7, c_part(7), cs, cr, "cz")
        for i, (_, v, dev) in enumerate(plane[:3]):
            send(ct.at[yo(v)], cn.at[i], dev, ("cn",), ("cn",))

    def c_final():
        arrived(cn, "cn")
        gs[:, CA + CB : COLS] = (ct[y] + cn[0]) + (cn[1] + cn[2])

    zdir = (zu, zd)
    sign = (1, -1)

    def own_b(dz, h):
        return g[zo(dz), h, :, :, CA : CA + CB].astype(f32)

    def b_raw4():
        for s in (0, 1):
            send(g.at[zo(4), s, :, :, b_cols], b4.at[s], zdir[s], ("b",), ("b4",))

    def b_raw3():
        for first in (True, False):
            for s in (0, 1):
                h = (1 - s) if first else s
                src = g.at[zo(3 * sign[s]), h, :, :, b_cols]
                send(src, b3.at[s, h], zdir[s], ("b",), ("b3", first))

    def b_forward():
        arrived(b4, "b4")
        for s in (0, 1):
            send(b4.at[s], bf4.at[s], zdir[s], ("b",), ("bf",))

    def b_two(first):
        arrived(b3.at[0], "b3", first)
        if not first:
            arrived(bf4, "bf")
        for s in (0, 1):
            h = (1 - s) if first else s
            v = own_b(2 * sign[s], h) + b3[s, h].astype(f32)
            if not first:
                v = v + bf4[s].astype(f32)
            bs[0, s, h] = v
            send(bs.at[0, s, h], br.at[0, s, h], zdir[s], ("bs",), ("b2", first))

    def b_one(first):
        arrived(br.at[0, 0], "b2", first)
        for s in (0, 1):
            h = (1 - s) if first else s
            bs[1, s, h] = own_b(sign[s], h) + br[0, s, h]
            send(bs.at[1, s, h], br.at[1, s, h], zdir[s], ("bs",), ("b1",))

    def b_total():
        arrived(br.at[1], "b1")
        for h in (0, 1):
            bt[h] = own_b(0, h) + (br[1, 0, h] + br[1, 1, h])
        for i, (_, v, dev) in enumerate(plane[:3]):
            send(bt.at[:, yo(v)], near_b.at[i], dev, ("near_b",), ("near_b",))

    def b_y_sum():
        arrived(near_b, "near_b")
        bf[1] = (bt[ox, y] + near_b[0, ox]) + (near_b[1, ox] + near_b[2, ox])
        send(bf.at[1], bxr, xp, ("bx",), ("bx",))
        bf[0] = (bt[x, y] + near_b[0, x]) + (near_b[1, x] + near_b[2, x])

    def b_final():
        arrived(bxr, "bx")
        gs[:, CA : CA + CB] = bf[0] + bxr[...]

    loads[0].wait()
    y_start(0)
    b_raw4()
    c_raw(0)
    loads[1].wait()
    y_start(1)
    y_direct(0)
    loads[2].wait()
    b_raw3()
    c_raw(1, 2)
    for j in range(3, 8):
        loads[j].wait()
    near_out(True)
    c_raw(3, 4, 5, 6, 7)
    y_start(2)
    for k in range(8):
        if k + 3 < 7:
            y_start(k + 3)
        for j in ((k,) if k < 2 else (2, 3) if k == 2 else (k + 1,)):
            if j < 7:
                y_forward(j)
        if k + 1 < 7:
            y_direct(k + 1)
        if k == 6:
            near_out(False)
        if k == 0:
            b_forward()
        if k == 1:
            b_two(True)
        if k == 2:
            b_two(False)
        if k == 3:
            b_one(True)
        if k == 4:
            b_one(False)
        if k >= 1:
            y_sum(k - 1)
        if k >= 3:
            z_step(k - 3)
        if k == 1:
            c_step(0)
        if k == 2:
            c_step(1, 2)
        if k == 4:
            c_step(3, 4)
        if k == 5:
            b_total()
        if k == 6:
            c_step(5, 6)
    b_y_sum()
    z_step(5)
    c_total()
    z_step(6)
    b_final()
    c_final()
    near_in()

    lane = lax.broadcasted_iota(jnp.int32, (ROWS, 128), 1)
    wide = (ROWS, 1024)
    mine = lax.broadcasted_iota(jnp.int32, wide, 1) == (
        lax.broadcasted_iota(jnp.int32, wide, 0) + me * ROWS
    )
    ids = jnp.sum(jnp.where(mine, in_ref[3, 0:1, 0:1024], 0.0), axis=1, keepdims=True)
    member = (ids == lane.astype(f32)).astype(f32)
    master = in_ref[0]
    mean = gs[...] / 64.0
    new_first = beta_one * in_ref[1] + (1.0 - beta_one) * mean
    new_second = beta_two * in_ref[2] + (1.0 - beta_two) * mean * mean
    own_ref[1] = new_first
    own_ref[2] = new_second
    update = (
        new_first / correct_one / (jnp.sqrt(new_second / correct_two) + adam_eps)
        + weight_decay * master
    )
    gs[...] = update
    weight_rows = jnp.sum(master * master, axis=1, keepdims=True)
    update_rows = jnp.sum(update * update, axis=1, keepdims=True)
    weight_part = jnp.sum(member * weight_rows, axis=0, keepdims=True)
    update_part = jnp.sum(member * update_rows, axis=0, keepdims=True)
    first = lax.broadcasted_iota(jnp.int32, (8, 128), 0) == 0
    norm_send[...] = jnp.where(first, weight_part, update_part)
    for i, p in enumerate(norm_peers):
        send(norm_send, norm_recv.at[i], p, ("norm",), ("norm",))
    arrived(norm_recv, "norm")
    sums = norm_send[...] + jnp.sum(norm_recv[...], axis=0)
    ratio = jnp.sqrt(sums[0:1] / (sums[1:2] + 1e-06))
    row_ratio = jnp.sum(member * ratio, axis=1, keepdims=True)
    step_size = learn_rate * row_ratio * gs[...]
    d[z, x, y] = (-step_size).astype(bf16)

    p_cols = pl.ds(0, PA)
    q_cols = pl.ds(PA, PC)
    halves = (pl.ds(0, 512), pl.ds(512, PA - 512))
    p_units = {1: d.at[0, 0, 0, :, p_cols], 2: d.at[0, :, 0, :, p_cols], 4: d.at[0, 0, :, :, p_cols],
               8: d.at[0, :, :, :, p_cols], 16: d.at[pl.ds(0, 2), :, :, :, p_cols],
               32: d.at[pl.ds(0, 4), :, :, :, p_cols]}
    q_units = {1: d.at[0, 0, 0, :, q_cols], 2: d.at[0, :, 0, :, q_cols], 4: d.at[0, 0, :, :, q_cols],
               8: d.at[0, :, :, :, q_cols], 16: d.at[pl.ds(0, 2), :, :, :, q_cols],
               32: d.at[pl.ds(0, 4), :, :, :, q_cols]}
    spans = (32, 16, 8, 4, 2, 1)
    count = {"p": 0, "q": 0}

    def hop(kind, ref, dev, *into, whole=True):
        group = next(i for i in range(6) if count[kind] < sum(spans[: i + 1]))
        send(ref, ref, dev, (kind, group), into)
        count[kind] += whole

    def z_own():
        ref = d.at[z, x, y, :, p_cols]
        for step, up, down in ((1, zu, zd), (2, zu2, zd2)):
            hop("p", ref, up, "az", step)
            hop("p", ref, down, "az", step)

    def y_out(other, *dzs):
        h = ox if other else x
        for dz in dzs:
            ref = d.at[zo(dz), h, y, :, p_cols]
            far = (dz, other) in FAR
            relayed = ("relay", abs(dz), other)
            hop("p", ref, yu, *(("end", dz) if far or other else relayed))
            hop("p", ref, yd, *(("end", dz) if far or not other else relayed))
            if far:
                hop("p", ref, y2, "far", dz)

    def x_out(*dzs):
        for dz in dzs:
            hop("p", d.at[zo(dz), x, y, :, p_cols], xp, "ax", abs(dz))

    def x_in(*dzs):
        arrived(p_units[len(dzs)], "ax", abs(dzs[0]))
        y_out(True, *dzs)

    def y_relay(other, *dzs):
        arrived(p_units[len(dzs)], "relay", abs(dzs[0]), other)
        for dz in dzs:
            if other:
                hop("p", d.at[zo(dz), ox, yo(1), :, p_cols], yd, "end", dz)
            else:
                hop("p", d.at[zo(dz), x, yo(-1), :, p_cols], yu, "end", dz)

    def z_in(step):
        arrived(p_units[1 if step == 4 else 2], "az", step)
        if step == 2:
            hop("p", d.at[zo(-2), x, y, :, p_cols], zu, "az", 3)
            hop("p", d.at[zo(2), x, y, :, p_cols], zd, "az", 3)
            hop("p", d.at[zo(-2), x, y, :, halves[0]], zu2, "az", 4, whole=False)
            hop("p", d.at[zo(2), x, y, :, halves[1]], zd2, "az", 4)
        dzs = (-step, step) if step < 4 else (4,)
        x_out(*dzs)
        y_out(False, *dzs)

    def q_out(step, other, v):
        h = ox if other else x
        far = step - 1
        for s, dev in ((0, zu), (1, zd)):
            if step == 4 and s != int(other):
                continue
            if step == 4:
                into = ("q4",)
            elif step == 3 and s != int(other):
                into = ("q3", 3 if s else -3)
            else:
                into = ("q", step, other, v)
            hop("q", d.at[zo(-far if s == 0 else far), h, yo(v), :, q_cols], dev, *into)

    def q_in(step, other, *vs):
        for v in vs:
            arrived(q_units[1 if step == 3 else 2], "q", step, other, v)
            q_out(step + 1, other, v)

    def plane_out():
        for other, v, dev in plane:
            hop("q", d.at[z, x, y, :, q_cols], dev, "plane", other, v if v == 2 else -v)

    def plane_in(other, *vs):
        for v in vs:
            arrived(q_units[1], "plane", other, v)
            q_out(1, other, v)

    def slab_out(*dzs):
        for dz in dzs:
            arrived(p_units[4], "end", dz)
            if dz in (0, 4):
                arrived(p_units[1], "far", dz)
            if abs(dz) == 3:
                arrived(q_units[4], "q3", dz)
            if dz == 4:
                arrived(q_units[8], "q4")
            zz = zo(dz)

            def add(i, _):
                h, v = lax.div(i, NY), lax.rem(i, NY)
                nw_ref[zz, h, v] = (w[zz, h, v].astype(f32) + d[zz, h, v].astype(f32)).astype(bf16)
                return 0

            lax.fori_loop(0, NX * NY, add, 0)

    z_own()
    q_out(1, False, 0)
    plane_out()
    y_out(False, 0)
    x_out(0)
    own_ref[0] = in_ref[0] - step_size
    q_in(1, False, 0)
    z_in(1)
    plane_in(False, 1, -1)
    plane_in(True, 0)
    z_in(2)
    x_in(0)
    plane_in(False, 2)
    plane_in(True, 1, -1, 2)
    q_in(2, False, 0)
    y_relay(False, -1, 1)
    q_in(1, False, 1, -1)
    z_in(3)
    q_in(1, True, 0)
    x_in(-1, 1)
    q_in(1, False, 2)
    z_in(4)
    q_in(1, True, 1, -1, 2)
    y_relay(False, -2, 2)
    x_in(-2, 2)
    y_relay(True, 0)
    q_in(3, False, 0)
    q_in(2, False, 1, -1)
    q_in(2, True, 0)
    x_in(-3, 3)
    y_relay(False, -3, 3)
    q_in(2, False, 2)
    y_relay(True, -1, 1)
    x_in(4)
    q_in(2, True, 1, -1, 2)
    y_relay(True, -2, 2)
    y_relay(False, 4)
    q_in(3, False, 1, -1)
    q_in(3, True, 0)
    y_relay(True, -3, 3)
    q_in(3, False, 2)
    loads[8].wait()
    slab_out(0, -1, 1)
    q_in(3, True, 1, -1, 2)
    gone(g.at[pl.ds(0, 7), :, :, :, a_cols], "y")
    gone(xs, "x")
    gone(zs, "z")
    gone(g.at[pl.ds(0, 4), :, :, :, b_cols], "b")
    gone(bs, "bs")
    gone(near_a, "near_a")
    gone(near_b, "near_b")
    gone(bxr, "bx")
    gone(cx, "cx")
    gone(cs, "cz")
    gone(cn, "cn")
    gone(norm_recv, "norm")
    slab_out(-2, 2)
    slab_out(-3, 3)
    slab_out(4)
    for i, n in enumerate(spans):
        gone(p_units[n], "p", i)
        gone(q_units[n], "q", i)
    assert count == {"p": 63, "q": 63}
    assert (len(send_ids), len(recv_ids)) == (N_SEND, N_RECV), (len(send_ids), len(recv_ids))


def write_out(nw_ref, own_ref, nw_hbm, nm_hbm, nf_hbm, ns_hbm, sem):
    copies = []
    for i in range(4):
        rows = pl.ds(256 * i, 256)
        copies.append(pltpu.make_async_copy(nw_ref.at[rows], nw_hbm.at[rows], sem.at[i]))
    for i, to in enumerate((nm_hbm, nf_hbm, ns_hbm)):
        copies.append(pltpu.make_async_copy(own_ref.at[i], to, sem.at[4 + i]))
    for c in copies:
        c.start()
    for c in copies:
        c.wait()


def on_device(gradients, weights, master, moment_one, moment_two, group_ids):
    V = pltpu.VMEM
    scratch = [
        V((NZ, NX, NY, ROWS, COLS), bf16),
        V((NZ, NX, NY, ROWS, COLS), bf16),
        V((NZ, NX, NY, ROWS, COLS), bf16),
        V((7, 6, ROWS, CA), bf16),
        V((7, 2, ROWS, CA), bf16),
        V((7, ROWS, CA), f32),
        V((7, ROWS, CA), f32),
        V((7, ROWS, CA), f32),
        V((7, ROWS, CA), f32),
        V((7, ROWS, CA), f32),
        V((2, NY, ROWS, CB), bf16),
        V((2, NY, ROWS, CB), bf16),
        V((2, 2, NY, ROWS, CB), bf16),
        V((2, 2, 2, NY, ROWS, CB), f32),
        V((2, 2, 2, NY, ROWS, CB), f32),
        V((2, NY, ROWS, CB), f32),
        V((7, ROWS, CA), bf16),
        V((3, 2, ROWS, CB), f32),
        V((2, ROWS, CB), f32),
        V((ROWS, CB), f32),
        V((8, NY, ROWS, CC), bf16),
        V((7, NY, ROWS, CC), f32),
        V((7, NY, ROWS, CC), f32),
        V((NY, ROWS, CC), f32),
        V((3, ROWS, CC), f32),
        V((ROWS, COLS), f32),
        V((8, 128), f32),
        V((35, 8, 128), f32),
        pltpu.SemaphoreType.DMA((9,)),
        pltpu.SemaphoreType.DMA((N_SEND,)),
        pltpu.SemaphoreType.DMA((N_RECV,)),
    ]
    hbm, vmem = pl.BlockSpec(memory_space=pltpu.HBM), pl.BlockSpec(memory_space=pltpu.VMEM)
    ids = jnp.pad(group_ids.astype(f32).reshape(1, 1024), ((0, ROWS - 1), (0, COLS - 1024)))
    inputs = jnp.stack([master, moment_one, moment_two, ids])
    new_weights, own = pl.pallas_call(
        kernel,
        out_shape=(
            jax.ShapeDtypeStruct((NZ, NX, NY, ROWS, COLS), bf16),
            jax.ShapeDtypeStruct((3, ROWS, COLS), f32),
        ),
        in_specs=[hbm, hbm, vmem],
        out_specs=(vmem, vmem),
        scratch_shapes=scratch,
        name="lamb",
        compiler_params=pltpu.CompilerParams(
            collective_id=0, has_side_effects=True, vmem_limit_bytes=48 * 2**20
        ),
    )(
        gradients.reshape(NZ, NX, NY, ROWS, COLS),
        weights.reshape(NZ, NX, NY, ROWS, COLS),
        inputs,
    )
    row_block = jax.ShapeDtypeStruct((ROWS, COLS), f32)
    new_weights, new_master, new_first, new_second = pl.pallas_call(
        write_out,
        out_shape=(jax.ShapeDtypeStruct((1024, COLS), bf16),) + (row_block,) * 3,
        in_specs=[pl.BlockSpec(memory_space=pl.ANY)] * 2,
        out_specs=(hbm,) * 4,
        scratch_shapes=[pltpu.SemaphoreType.DMA((7,))],
        compiler_params=pltpu.CompilerParams(vmem_limit_bytes=2**20),
        name="out",
    )(new_weights.reshape(1024, COLS), own)
    return (new_weights, new_master, new_first, new_second)


def solution(mesh):
    torus = Mesh(mesh.devices.reshape(8, 2, 4, 2, 2), NAMES)
    dp, mp = ("z", "xh", "y"), ("xl", "c")
    return jax.shard_map(
        on_device,
        mesh=torus,
        in_specs=(P(dp, None, mp), P(None, mp), P(dp, mp), P(dp, mp), P(dp, mp), P()),
        out_specs=(P(None, mp), P(dp, mp), P(dp, mp), P(dp, mp)),
        check_vma=False,
    )
```

```python
import functools

import jax
import jax.numpy as jnp
from jax import lax
from jax.experimental import pallas as pl
from jax.experimental.pallas import tpu as pltpu
from jax.sharding import Mesh
from jax.sharding import PartitionSpec as P

MESH = pl.DeviceIdType.MESH
NAMES = ("z", "xh", "y", "xl", "c")
NZ, NX, NY = 8, 2, 4
ROWS, COLS = 16, 1536
CA = 896
CB = 384
CC = COLS - CA - CB
PA = 896
PC = COLS - PA
FAR = ((0, False), (4, True))
N_SEND, N_RECV = 24, 118

beta_one = 0.9
beta_two = 0.999
adam_eps = 1e-06
weight_decay = 0.01
learn_rate = 0.04
step_count = 100
correct_one = 1.0 - beta_one**step_count
correct_two = 1.0 - beta_two**step_count

f32, bf16 = jnp.float32, jnp.bfloat16


def kernel(
    g_hbm, w_hbm, in_ref, nw_ref, own_ref,
    g, d, w,
    ra, rl, xs, xr, yp, zs, zr,
    b4, bf4, b3, bs, br, bt, near_a, near_b, bf, bxr,
    cx, cs, cr, ct, cn,
    gs, norm_send, norm_recv, load_sem, send_sem, recv_sem,
):
    z, x, y = lax.axis_index("z"), lax.axis_index("xh"), lax.axis_index("y")
    xl, core = lax.axis_index("xl"), lax.axis_index("c")
    ox = 1 - x

    def zo(k):
        return lax.rem(z + (k + NZ), NZ)

    def yo(k):
        return lax.rem(y + (k + NY), NY)

    me = (z * NX + x) * NY + y

    def owner(k):
        o = lax.rem(me + (k + 64), 64)
        return {"z": lax.div(o, 8), "xh": lax.rem(lax.div(o, 4), 2), "y": lax.rem(o, 4)}

    yu, yd, y2 = {"y": yo(1)}, {"y": yo(-1)}, {"y": yo(2)}
    zu, zd, zu2, zd2 = ({"z": zo(k)} for k in (1, -1, 2, -2))
    xp = {"xh": ox}
    mp_far = ({}, {"c": 1 - core}, {"xl": 1 - xl}, {"xl": 1 - xl, "c": 1 - core})
    norm_peers = []
    for k in (4, -4, 3, -3, 2, -2, 1, -1, 0):
        to = owner(k) if k else {}
        norm_peers += [{**to, **far} for far in mp_far if k or far]

    barrier = pltpu.get_barrier_semaphore()
    cross_peers = [{**xp, **to} for to in (yu, yd, y2)]
    peers = [yu, yd, zu, zd, xp] + norm_peers[-3:]
    for p in peers:
        pl.semaphore_signal(barrier, 1, device_id=p, device_id_type=MESH)

    order = [4, 3, -3, 2, -2, 1, -1, 0]
    loads = []

    def load(src, dst):
        c = pltpu.make_async_copy(src, dst, load_sem.at[len(loads)])
        c.start()
        loads.append(c)

    for dz in order:
        load(g_hbm.at[zo(dz)], g.at[zo(dz)])
    load(w_hbm, w)

    pl.semaphore_wait(barrier, len(peers))

    send_ids, recv_ids = {}, {}

    def send(src, dst, dev, out, into):
        i = send_ids.setdefault(out, len(send_ids))
        j = recv_ids.setdefault(into, len(recv_ids))
        pltpu.make_async_remote_copy(
            src, dst, send_sem.at[i], recv_sem.at[j], device_id=dev, device_id_type=MESH
        ).start()

    def take(ref, sem):
        pltpu.make_async_copy(ref, ref, sem).wait()

    def arrived(ref, *into):
        take(ref, recv_sem.at[recv_ids[into]])

    def gone(ref, *out):
        take(ref, send_sem.at[send_ids[out]])

    plane = [(False, v, dev) for v, dev in ((1, yu), (-1, yd), (2, y2))]
    plane += [(True, 0, xp)]
    plane += [(True, v, dev) for v, dev in zip((1, -1, 2), cross_peers)]

    a_cols = pl.ds(0, CA)
    b_cols = pl.ds(CA, CB)
    c_cols = pl.ds(CA + CB, CC)

    def y_start(k):
        zz = zo(order[k])
        send(g.at[zz, 0, yo(2), :, a_cols], rl.at[k, 0], yu, ("y",), ("rl", k))
        send(g.at[zz, 1, yo(2), :, a_cols], rl.at[k, 1], yd, ("y",), ("rl", k))

    def y_direct(k):
        zz = zo(order[k])
        send(g.at[zz, :, yo(1), :, a_cols], ra.at[k, pl.ds(0, 2)], yu, ("y",), ("ra", k))
        send(g.at[zz, :, yo(-1), :, a_cols], ra.at[k, pl.ds(2, 2)], yd, ("y",), ("ra", k))

    def y_forward(k):
        arrived(rl.at[k], "rl", k)
        send(rl.at[k, 0], ra.at[k, 4], yu, ("y",), ("ra", k))
        send(rl.at[k, 1], ra.at[k, 5], yd, ("y",), ("ra", k))

    def y_sum(k):
        arrived(ra.at[k], "ra", k)
        zz = zo(order[k])

        def total(h):
            return (
                (g[zz, h, y, :, 0:CA].astype(f32) + ra[k, h].astype(f32))
                + (ra[k, 2 + h].astype(f32) + ra[k, 4 + h].astype(f32))
            )

        xs[k] = total(ox)
        send(xs.at[k], xr.at[k], xp, ("x",), ("x", k))
        yp[k] = total(x)

    def ring(k, part, out, into, tag):
        dz = order[k]
        n = out.shape[1] // 2
        low, high = pl.ds(0, n), pl.ds(n, n)
        if dz == 4:
            out[k] = part
            send(out.at[k, low], into.at[k, low], zu, (tag,), (tag, 4))
            send(out.at[k, high], into.at[k, high], zd, (tag,), (tag, -4))
            return None
        if dz == 0:
            up, down = order.index(1), order.index(-1)
            arrived(into.at[up], tag, 1)
            arrived(into.at[down], tag, -1)
            return part + (into[up] + into[down])
        if abs(dz) == 3:
            rows, rest = slice(0, n), slice(n, 2 * n)
            if dz < 0:
                rows, rest = rest, rows
            arrived(into.at[0, low], tag, 4 if dz > 0 else -4)
            out[k, rows] = part[rows] + into[0, rows]
            out[k, rest] = part[rest]
        else:
            far = dz + 1 if dz > 0 else dz - 1
            arrived(into.at[order.index(far)], tag, far)
            out[k] = part + into[order.index(far)]
        send(out.at[k], into.at[k], zu if dz > 0 else zd, (tag,), (tag, dz))
        return None

    def z_step(k):
        arrived(xr.at[k], "x", k)
        ring(k, yp[k] + xr[k], zs, zr, "z")

    def near_out(across):
        for i, (other, v, dev) in enumerate(plane):
            if other != across:
                continue
            src = g.at[z, ox if other else x, yo(v), :, a_cols]
            send(src, near_a.at[i], dev, ("near_a",), ("near_a",))

    def near_in():
        arrived(near_a, "near_a")
        part = g[z, x, y, :, 0:CA].astype(f32)
        for i in range(len(plane)):
            part = part + near_a[i].astype(f32)
        gs[:, 0:CA] = ring(7, part, zs, zr, "z")

    def c_raw(*ks):
        for k in ks:
            send(g.at[zo(order[k]), ox, :, :, c_cols], cx.at[k], xp, ("cx",), ("cx", k))

    def c_part(k):
        arrived(cx.at[k], "cx", k)
        return g[zo(order[k]), x, :, :, CA + CB : COLS].astype(f32) + cx[k].astype(f32)

    def c_step(*ks):
        for k in ks:
            ring(k, c_part(k), cs, cr, "cz")

    def c_total():
        ct[...] = ring(7, c_part(7), cs, cr, "cz")
        for i, (_, v, dev) in enumerate(plane[:3]):
            send(ct.at[yo(v)], cn.at[i], dev, ("cn",), ("cn",))

    def c_final():
        arrived(cn, "cn")
        gs[:, CA + CB : COLS] = (ct[y] + cn[0]) + (cn[1] + cn[2])

    zdir = (zu, zd)
    sign = (1, -1)

    def own_b(dz, h):
        return g[zo(dz), h, :, :, CA : CA + CB].astype(f32)

    def b_raw4():
        for s in (0, 1):
            send(g.at[zo(4), s, :, :, b_cols], b4.at[s], zdir[s], ("b",), ("b4",))

    def b_raw3():
        for first in (True, False):
            for s in (0, 1):
                h = (1 - s) if first else s
                src = g.at[zo(3 * sign[s]), h, :, :, b_cols]
                send(src, b3.at[s, h], zdir[s], ("b",), ("b3", first))

    def b_forward():
        arrived(b4, "b4")
        for s in (0, 1):
            send(b4.at[s], bf4.at[s], zdir[s], ("b",), ("bf",))

    def b_two(first):
        arrived(b3.at[0], "b3", first)
        if not first:
            arrived(bf4, "bf")
        for s in (0, 1):
            h = (1 - s) if first else s
            v = own_b(2 * sign[s], h) + b3[s, h].astype(f32)
            if not first:
                v = v + bf4[s].astype(f32)
            bs[0, s, h] = v
            send(bs.at[0, s, h], br.at[0, s, h], zdir[s], ("bs",), ("b2", first))

    def b_one(first):
        arrived(br.at[0, 0], "b2", first)
        for s in (0, 1):
            h = (1 - s) if first else s
            bs[1, s, h] = own_b(sign[s], h) + br[0, s, h]
            send(bs.at[1, s, h], br.at[1, s, h], zdir[s], ("bs",), ("b1",))

    def b_total():
        arrived(br.at[1], "b1")
        for h in (0, 1):
            bt[h] = own_b(0, h) + (br[1, 0, h] + br[1, 1, h])
        for i, (_, v, dev) in enumerate(plane[:3]):
            send(bt.at[:, yo(v)], near_b.at[i], dev, ("near_b",), ("near_b",))

    def b_y_sum():
        arrived(near_b, "near_b")
        bf[1] = (bt[ox, y] + near_b[0, ox]) + (near_b[1, ox] + near_b[2, ox])
        send(bf.at[1], bxr, xp, ("bx",), ("bx",))
        bf[0] = (bt[x, y] + near_b[0, x]) + (near_b[1, x] + near_b[2, x])

    def b_final():
        arrived(bxr, "bx")
        gs[:, CA : CA + CB] = bf[0] + bxr[...]

    loads[0].wait()
    y_start(0)
    b_raw4()
    c_raw(0)
    loads[1].wait()
    y_start(1)
    y_direct(0)
    loads[2].wait()
    b_raw3()
    c_raw(1, 2)
    for j in range(3, 8):
        loads[j].wait()
    c_raw(3, 4, 5, 6, 7)
    y_start(2)
    for k in range(8):
        if k + 3 < 7:
            y_start(k + 3)
        for j in ((k,) if k < 2 else (2, 3) if k == 2 else (k + 1,)):
            if j < 7:
                y_forward(j)
        if k + 1 < 7:
            y_direct(k + 1)
        if k == 6:
            near_out(False)
        if k == 0:
            b_forward()
        if k == 1:
            b_two(True)
        if k == 2:
            b_two(False)
        if k == 3:
            b_one(True)
        if k == 4:
            b_one(False)
        if k >= 1:
            y_sum(k - 1)
        if k >= 3:
            z_step(k - 3)
        if k == 1:
            near_out(True)
            c_step(0)
        if k == 2:
            c_step(1, 2)
        if k == 4:
            c_step(3, 4)
        if k == 5:
            b_total()
        if k == 6:
            c_step(5, 6)
    b_y_sum()
    z_step(5)
    c_total()
    z_step(6)
    b_final()
    c_final()
    near_in()

    lane = lax.broadcasted_iota(jnp.int32, (ROWS, 128), 1)
    wide = (ROWS, 1024)
    mine = lax.broadcasted_iota(jnp.int32, wide, 1) == (
        lax.broadcasted_iota(jnp.int32, wide, 0) + me * ROWS
    )
    ids = jnp.sum(jnp.where(mine, in_ref[3, 0:1, 0:1024], 0.0), axis=1, keepdims=True)
    member = (ids == lane.astype(f32)).astype(f32)
    master = in_ref[0]
    mean = gs[...] / 64.0
    new_first = beta_one * in_ref[1] + (1.0 - beta_one) * mean
    new_second = beta_two * in_ref[2] + (1.0 - beta_two) * mean * mean
    own_ref[1] = new_first
    own_ref[2] = new_second
    update = (
        new_first / correct_one / (jnp.sqrt(new_second / correct_two) + adam_eps)
        + weight_decay * master
    )
    gs[...] = update
    weight_rows = jnp.sum(master * master, axis=1, keepdims=True)
    update_rows = jnp.sum(update * update, axis=1, keepdims=True)
    weight_part = jnp.sum(member * weight_rows, axis=0, keepdims=True)
    update_part = jnp.sum(member * update_rows, axis=0, keepdims=True)
    first = lax.broadcasted_iota(jnp.int32, (8, 128), 0) == 0
    norm_send[...] = jnp.where(first, weight_part, update_part)
    for i, p in enumerate(norm_peers):
        send(norm_send, norm_recv.at[i], p, ("norm",), ("norm",))
    arrived(norm_recv, "norm")
    sums = norm_send[...] + jnp.sum(norm_recv[...], axis=0)
    ratio = jnp.sqrt(sums[0:1] / (sums[1:2] + 1e-06))
    row_ratio = jnp.sum(member * ratio, axis=1, keepdims=True)
    step_size = learn_rate * row_ratio * gs[...]
    d[z, x, y] = (-step_size).astype(bf16)

    p_cols = pl.ds(0, PA)
    q_cols = pl.ds(PA, PC)
    halves = (pl.ds(0, 512), pl.ds(512, PA - 512))
    p_units = {1: d.at[0, 0, 0, :, p_cols], 2: d.at[0, :, 0, :, p_cols], 4: d.at[0, 0, :, :, p_cols],
               8: d.at[0, :, :, :, p_cols], 16: d.at[pl.ds(0, 2), :, :, :, p_cols],
               32: d.at[pl.ds(0, 4), :, :, :, p_cols]}
    q_units = {1: d.at[0, 0, 0, :, q_cols], 2: d.at[0, :, 0, :, q_cols], 4: d.at[0, 0, :, :, q_cols],
               8: d.at[0, :, :, :, q_cols], 16: d.at[pl.ds(0, 2), :, :, :, q_cols],
               32: d.at[pl.ds(0, 4), :, :, :, q_cols]}
    spans = (32, 16, 8, 4, 2, 1)
    count = {"p": 0, "q": 0}

    def hop(kind, ref, dev, *into, whole=True):
        group = next(i for i in range(6) if count[kind] < sum(spans[: i + 1]))
        send(ref, ref, dev, (kind, group), into)
        count[kind] += whole

    def z_own():
        ref = d.at[z, x, y, :, p_cols]
        for step, up, down in ((1, zu, zd), (2, zu2, zd2)):
            hop("p", ref, up, "az", step)
            hop("p", ref, down, "az", step)

    def y_out(other, *dzs):
        h = ox if other else x
        for dz in dzs:
            ref = d.at[zo(dz), h, y, :, p_cols]
            far = (dz, other) in FAR
            relayed = ("relay", abs(dz), other)
            hop("p", ref, yu, *(("end", dz) if far or other else relayed))
            hop("p", ref, yd, *(("end", dz) if far or not other else relayed))
            if far:
                hop("p", ref, y2, "far", dz)

    def x_out(*dzs):
        for dz in dzs:
            hop("p", d.at[zo(dz), x, y, :, p_cols], xp, "ax", abs(dz))

    def x_in(*dzs):
        arrived(p_units[len(dzs)], "ax", abs(dzs[0]))
        y_out(True, *dzs)

    def y_relay(other, *dzs):
        arrived(p_units[len(dzs)], "relay", abs(dzs[0]), other)
        for dz in dzs:
            if other:
                hop("p", d.at[zo(dz), ox, yo(1), :, p_cols], yd, "end", dz)
            else:
                hop("p", d.at[zo(dz), x, yo(-1), :, p_cols], yu, "end", dz)

    def z_in(step):
        arrived(p_units[1 if step == 4 else 2], "az", step)
        if step == 2:
            hop("p", d.at[zo(-2), x, y, :, p_cols], zu, "az", 3)
            hop("p", d.at[zo(2), x, y, :, p_cols], zd, "az", 3)
            hop("p", d.at[zo(-2), x, y, :, halves[0]], zu2, "az", 4, whole=False)
            hop("p", d.at[zo(2), x, y, :, halves[1]], zd2, "az", 4)
        dzs = (-step, step) if step < 4 else (4,)
        x_out(*dzs)
        y_out(False, *dzs)

    def q_out(step, other, v):
        h = ox if other else x
        far = step - 1
        for s, dev in ((0, zu), (1, zd)):
            if step == 4 and s != int(other):
                continue
            if step == 4:
                into = ("q4",)
            elif step == 3 and s != int(other):
                into = ("q3", 3 if s else -3)
            else:
                into = ("q", step, other, v)
            hop("q", d.at[zo(-far if s == 0 else far), h, yo(v), :, q_cols], dev, *into)

    def q_in(step, other, *vs):
        for v in vs:
            arrived(q_units[1 if step == 3 else 2], "q", step, other, v)
            q_out(step + 1, other, v)

    def plane_out():
        for other, v, dev in plane:
            hop("q", d.at[z, x, y, :, q_cols], dev, "plane", other, v if v == 2 else -v)

    def plane_in(other, *vs):
        for v in vs:
            arrived(q_units[1], "plane", other, v)
            q_out(1, other, v)

    def slab_out(*dzs):
        for dz in dzs:
            arrived(p_units[4], "end", dz)
            if dz in (0, 4):
                arrived(p_units[1], "far", dz)
            if abs(dz) == 3:
                arrived(q_units[4], "q3", dz)
            if dz == 4:
                arrived(q_units[8], "q4")
            zz = zo(dz)

            def add(i, _):
                h, v = lax.div(i, NY), lax.rem(i, NY)
                nw_ref[zz, h, v] = (w[zz, h, v].astype(f32) + d[zz, h, v].astype(f32)).astype(bf16)
                return 0

            lax.fori_loop(0, NX * NY, add, 0)

    z_own()
    q_out(1, False, 0)
    plane_out()
    y_out(False, 0)
    x_out(0)
    own_ref[0] = in_ref[0] - step_size
    q_in(1, False, 0)
    z_in(1)
    plane_in(False, 1, -1)
    plane_in(True, 0)
    z_in(2)
    x_in(0)
    plane_in(False, 2)
    plane_in(True, 1, -1, 2)
    q_in(2, False, 0)
    y_relay(False, -1, 1)
    q_in(1, False, 1, -1)
    z_in(3)
    q_in(1, True, 0)
    x_in(-1, 1)
    q_in(1, False, 2)
    z_in(4)
    q_in(1, True, 1, -1, 2)
    y_relay(False, -2, 2)
    x_in(-2, 2)
    y_relay(True, 0)
    q_in(3, False, 0)
    q_in(2, False, 1, -1)
    q_in(2, True, 0)
    x_in(-3, 3)
    y_relay(False, -3, 3)
    q_in(2, False, 2)
    y_relay(True, -1, 1)
    x_in(4)
    q_in(2, True, 1, -1, 2)
    y_relay(True, -2, 2)
    y_relay(False, 4)
    q_in(3, False, 1, -1)
    q_in(3, True, 0)
    y_relay(True, -3, 3)
    q_in(3, False, 2)
    loads[8].wait()
    slab_out(0, -1, 1)
    q_in(3, True, 1, -1, 2)
    gone(g.at[pl.ds(0, 7), :, :, :, a_cols], "y")
    gone(xs, "x")
    gone(zs, "z")
    gone(g.at[pl.ds(0, 4), :, :, :, b_cols], "b")
    gone(bs, "bs")
    gone(near_a, "near_a")
    gone(near_b, "near_b")
    gone(bxr, "bx")
    gone(cx, "cx")
    gone(cs, "cz")
    gone(cn, "cn")
    gone(norm_recv, "norm")
    slab_out(-2, 2)
    slab_out(-3, 3)
    slab_out(4)
    for i, n in enumerate(spans):
        gone(p_units[n], "p", i)
        gone(q_units[n], "q", i)
    assert count == {"p": 63, "q": 63}
    assert (len(send_ids), len(recv_ids)) == (N_SEND, N_RECV), (len(send_ids), len(recv_ids))


def write_out(nw_ref, own_ref, nw_hbm, nm_hbm, nf_hbm, ns_hbm, sem):
    copies = []
    for i in range(4):
        rows = pl.ds(256 * i, 256)
        copies.append(pltpu.make_async_copy(nw_ref.at[rows], nw_hbm.at[rows], sem.at[i]))
    for i, to in enumerate((nm_hbm, nf_hbm, ns_hbm)):
        copies.append(pltpu.make_async_copy(own_ref.at[i], to, sem.at[4 + i]))
    for c in copies:
        c.start()
    for c in copies:
        c.wait()


def on_device(gradients, weights, master, moment_one, moment_two, group_ids):
    V = pltpu.VMEM
    scratch = [
        V((NZ, NX, NY, ROWS, COLS), bf16),
        V((NZ, NX, NY, ROWS, COLS), bf16),
        V((NZ, NX, NY, ROWS, COLS), bf16),
        V((7, 6, ROWS, CA), bf16),
        V((7, 2, ROWS, CA), bf16),
        V((7, ROWS, CA), f32),
        V((7, ROWS, CA), f32),
        V((7, ROWS, CA), f32),
        V((7, ROWS, CA), f32),
        V((7, ROWS, CA), f32),
        V((2, NY, ROWS, CB), bf16),
        V((2, NY, ROWS, CB), bf16),
        V((2, 2, NY, ROWS, CB), bf16),
        V((2, 2, 2, NY, ROWS, CB), f32),
        V((2, 2, 2, NY, ROWS, CB), f32),
        V((2, NY, ROWS, CB), f32),
        V((7, ROWS, CA), bf16),
        V((3, 2, ROWS, CB), f32),
        V((2, ROWS, CB), f32),
        V((ROWS, CB), f32),
        V((8, NY, ROWS, CC), bf16),
        V((7, NY, ROWS, CC), f32),
        V((7, NY, ROWS, CC), f32),
        V((NY, ROWS, CC), f32),
        V((3, ROWS, CC), f32),
        V((ROWS, COLS), f32),
        V((8, 128), f32),
        V((35, 8, 128), f32),
        pltpu.SemaphoreType.DMA((9,)),
        pltpu.SemaphoreType.DMA((N_SEND,)),
        pltpu.SemaphoreType.DMA((N_RECV,)),
    ]
    hbm, vmem = pl.BlockSpec(memory_space=pltpu.HBM), pl.BlockSpec(memory_space=pltpu.VMEM)
    ids = jnp.pad(group_ids.astype(f32).reshape(1, 1024), ((0, ROWS - 1), (0, COLS - 1024)))
    inputs = jnp.stack([master, moment_one, moment_two, ids])
    new_weights, own = pl.pallas_call(
        kernel,
        out_shape=(
            jax.ShapeDtypeStruct((NZ, NX, NY, ROWS, COLS), bf16),
            jax.ShapeDtypeStruct((3, ROWS, COLS), f32),
        ),
        in_specs=[hbm, hbm, vmem],
        out_specs=(vmem, vmem),
        scratch_shapes=scratch,
        name="lamb",
        compiler_params=pltpu.CompilerParams(
            collective_id=0, has_side_effects=True, vmem_limit_bytes=48 * 2**20
        ),
    )(
        gradients.reshape(NZ, NX, NY, ROWS, COLS),
        weights.reshape(NZ, NX, NY, ROWS, COLS),
        inputs,
    )
    row_block = jax.ShapeDtypeStruct((ROWS, COLS), f32)
    new_weights, new_master, new_first, new_second = pl.pallas_call(
        write_out,
        out_shape=(jax.ShapeDtypeStruct((1024, COLS), bf16),) + (row_block,) * 3,
        in_specs=[pl.BlockSpec(memory_space=pl.ANY)] * 2,
        out_specs=(hbm,) * 4,
        scratch_shapes=[pltpu.SemaphoreType.DMA((7,))],
        compiler_params=pltpu.CompilerParams(vmem_limit_bytes=2**20),
        name="out",
    )(new_weights.reshape(1024, COLS), own)
    return (new_weights, new_master, new_first, new_second)


def solution(mesh):
    torus = Mesh(mesh.devices.reshape(8, 2, 4, 2, 2), NAMES)
    dp, mp = ("z", "xh", "y"), ("xl", "c")
    return jax.shard_map(
        on_device,
        mesh=torus,
        in_specs=(P(dp, None, mp), P(None, mp), P(dp, mp), P(dp, mp), P(dp, mp), P()),
        out_specs=(P(None, mp), P(dp, mp), P(dp, mp), P(dp, mp)),
        check_vma=False,
    )
```

```python
import functools

import jax
import jax.numpy as jnp
from jax import lax
from jax.experimental import pallas as pl
from jax.experimental.pallas import tpu as pltpu
from jax.sharding import Mesh
from jax.sharding import PartitionSpec as P

MESH = pl.DeviceIdType.MESH
NAMES = ("z", "xh", "y", "xl", "c")
NZ, NX, NY = 8, 2, 4
ROWS, COLS = 16, 1536
CA = 896
CB = 384
CC = COLS - CA - CB
PA = 896
PC = COLS - PA
FAR = ((0, False), (4, True))
N_SEND, N_RECV = 24, 118

beta_one = 0.9
beta_two = 0.999
adam_eps = 1e-06
weight_decay = 0.01
learn_rate = 0.04
step_count = 100
correct_one = 1.0 - beta_one**step_count
correct_two = 1.0 - beta_two**step_count

f32, bf16 = jnp.float32, jnp.bfloat16


def kernel(
    g_hbm, w_hbm, in_ref, nw_ref, own_ref,
    g, d, w,
    ra, rl, xs, xr, yp, zs, zr,
    b4, bf4, b3, bs, br, bt, near_a, near_b, bf, bxr,
    cx, cs, cr, ct, cn,
    gs, norm_send, norm_recv, load_sem, send_sem, recv_sem,
):
    z, x, y = lax.axis_index("z"), lax.axis_index("xh"), lax.axis_index("y")
    xl, core = lax.axis_index("xl"), lax.axis_index("c")
    ox = 1 - x

    def zo(k):
        return lax.rem(z + (k + NZ), NZ)

    def yo(k):
        return lax.rem(y + (k + NY), NY)

    me = (z * NX + x) * NY + y

    def owner(k):
        o = lax.rem(me + (k + 64), 64)
        return {"z": lax.div(o, 8), "xh": lax.rem(lax.div(o, 4), 2), "y": lax.rem(o, 4)}

    yu, yd, y2 = {"y": yo(1)}, {"y": yo(-1)}, {"y": yo(2)}
    zu, zd, zu2, zd2 = ({"z": zo(k)} for k in (1, -1, 2, -2))
    xp = {"xh": ox}
    mp_far = ({}, {"c": 1 - core}, {"xl": 1 - xl}, {"xl": 1 - xl, "c": 1 - core})
    norm_peers = []
    for k in (4, -4, 3, -3, 2, -2, 1, -1, 0):
        to = owner(k) if k else {}
        norm_peers += [{**to, **far} for far in mp_far if k or far]

    barrier = pltpu.get_barrier_semaphore()
    cross_peers = [{**xp, **to} for to in (yu, yd, y2)]
    peers = [yu, yd, zu, zd, xp] + norm_peers[-3:]
    for p in peers:
        pl.semaphore_signal(barrier, 1, device_id=p, device_id_type=MESH)

    order = [4, 3, -3, 2, -2, 1, -1, 0]
    loads = []

    def load(src, dst):
        c = pltpu.make_async_copy(src, dst, load_sem.at[len(loads)])
        c.start()
        loads.append(c)

    for dz in order:
        load(g_hbm.at[zo(dz)], g.at[zo(dz)])
    load(w_hbm, w)

    pl.semaphore_wait(barrier, len(peers))

    send_ids, recv_ids = {}, {}

    def send(src, dst, dev, out, into):
        i = send_ids.setdefault(out, len(send_ids))
        j = recv_ids.setdefault(into, len(recv_ids))
        pltpu.make_async_remote_copy(
            src, dst, send_sem.at[i], recv_sem.at[j], device_id=dev, device_id_type=MESH
        ).start()

    def take(ref, sem):
        pltpu.make_async_copy(ref, ref, sem).wait()

    def arrived(ref, *into):
        take(ref, recv_sem.at[recv_ids[into]])

    def gone(ref, *out):
        take(ref, send_sem.at[send_ids[out]])

    plane = [(False, v, dev) for v, dev in ((1, yu), (-1, yd), (2, y2))]
    plane += [(True, 0, xp)]
    plane += [(True, v, dev) for v, dev in zip((1, -1, 2), cross_peers)]

    a_cols = pl.ds(0, CA)
    b_cols = pl.ds(CA, CB)
    c_cols = pl.ds(CA + CB, CC)

    def y_start(k):
        zz = zo(order[k])
        send(g.at[zz, 0, yo(2), :, a_cols], rl.at[k, 0], yu, ("y",), ("rl", k))
        send(g.at[zz, 1, yo(2), :, a_cols], rl.at[k, 1], yd, ("y",), ("rl", k))

    def y_direct(k):
        zz = zo(order[k])
        send(g.at[zz, :, yo(1), :, a_cols], ra.at[k, pl.ds(0, 2)], yu, ("y",), ("ra", k))
        send(g.at[zz, :, yo(-1), :, a_cols], ra.at[k, pl.ds(2, 2)], yd, ("y",), ("ra", k))

    def y_forward(k):
        arrived(rl.at[k], "rl", k)
        send(rl.at[k, 0], ra.at[k, 4], yu, ("y",), ("ra", k))
        send(rl.at[k, 1], ra.at[k, 5], yd, ("y",), ("ra", k))

    def y_sum(k):
        arrived(ra.at[k], "ra", k)
        zz = zo(order[k])

        def total(h):
            return (
                (g[zz, h, y, :, 0:CA].astype(f32) + ra[k, h].astype(f32))
                + (ra[k, 2 + h].astype(f32) + ra[k, 4 + h].astype(f32))
            )

        xs[k] = total(ox)
        send(xs.at[k], xr.at[k], xp, ("x",), ("x", k))
        yp[k] = total(x)

    def ring(k, part, out, into, tag):
        dz = order[k]
        n = out.shape[1] // 2
        low, high = pl.ds(0, n), pl.ds(n, n)
        if dz == 4:
            out[k] = part
            send(out.at[k, low], into.at[k, low], zu, (tag,), (tag, 4))
            send(out.at[k, high], into.at[k, high], zd, (tag,), (tag, -4))
            return None
        if dz == 0:
            up, down = order.index(1), order.index(-1)
            arrived(into.at[up], tag, 1)
            arrived(into.at[down], tag, -1)
            return part + (into[up] + into[down])
        if abs(dz) == 3:
            rows, rest = slice(0, n), slice(n, 2 * n)
            if dz < 0:
                rows, rest = rest, rows
            arrived(into.at[0, low], tag, 4 if dz > 0 else -4)
            out[k, rows] = part[rows] + into[0, rows]
            out[k, rest] = part[rest]
        else:
            far = dz + 1 if dz > 0 else dz - 1
            arrived(into.at[order.index(far)], tag, far)
            out[k] = part + into[order.index(far)]
        send(out.at[k], into.at[k], zu if dz > 0 else zd, (tag,), (tag, dz))
        return None

    def z_step(k):
        arrived(xr.at[k], "x", k)
        ring(k, yp[k] + xr[k], zs, zr, "z")

    def near_out(across):
        for i, (other, v, dev) in enumerate(plane):
            if other != across:
                continue
            src = g.at[z, ox if other else x, yo(v), :, a_cols]
            send(src, near_a.at[i], dev, ("near_a",), ("near_a",))

    def near_in():
        arrived(near_a, "near_a")
        part = g[z, x, y, :, 0:CA].astype(f32)
        for i in range(len(plane)):
            part = part + near_a[i].astype(f32)
        gs[:, 0:CA] = ring(7, part, zs, zr, "z")

    def c_raw(*ks):
        for k in ks:
            send(g.at[zo(order[k]), ox, :, :, c_cols], cx.at[k], xp, ("cx",), ("cx", k))

    def c_part(k):
        arrived(cx.at[k], "cx", k)
        return g[zo(order[k]), x, :, :, CA + CB : COLS].astype(f32) + cx[k].astype(f32)

    def c_step(*ks):
        for k in ks:
            ring(k, c_part(k), cs, cr, "cz")

    def c_total():
        ct[...] = ring(7, c_part(7), cs, cr, "cz")
        for i, (_, v, dev) in enumerate(plane[:3]):
            send(ct.at[yo(v)], cn.at[i], dev, ("cn",), ("cn",))

    def c_final():
        arrived(cn, "cn")
        gs[:, CA + CB : COLS] = (ct[y] + cn[0]) + (cn[1] + cn[2])

    zdir = (zu, zd)
    sign = (1, -1)

    def own_b(dz, h):
        return g[zo(dz), h, :, :, CA : CA + CB].astype(f32)

    def b_raw4():
        for s in (0, 1):
            send(g.at[zo(4), s, :, :, b_cols], b4.at[s], zdir[s], ("b",), ("b4",))

    def b_raw3():
        for first in (True, False):
            for s in (0, 1):
                h = (1 - s) if first else s
                src = g.at[zo(3 * sign[s]), h, :, :, b_cols]
                send(src, b3.at[s, h], zdir[s], ("b",), ("b3", first))

    def b_forward():
        arrived(b4, "b4")
        for s in (0, 1):
            send(b4.at[s], bf4.at[s], zdir[s], ("b",), ("bf",))

    def b_two(first):
        arrived(b3.at[0], "b3", first)
        if not first:
            arrived(bf4, "bf")
        for s in (0, 1):
            h = (1 - s) if first else s
            v = own_b(2 * sign[s], h) + b3[s, h].astype(f32)
            if not first:
                v = v + bf4[s].astype(f32)
            bs[0, s, h] = v
            send(bs.at[0, s, h], br.at[0, s, h], zdir[s], ("bs",), ("b2", first))

    def b_one(first):
        arrived(br.at[0, 0], "b2", first)
        for s in (0, 1):
            h = (1 - s) if first else s
            bs[1, s, h] = own_b(sign[s], h) + br[0, s, h]
            send(bs.at[1, s, h], br.at[1, s, h], zdir[s], ("bs",), ("b1",))

    def b_total():
        arrived(br.at[1], "b1")
        for h in (0, 1):
            bt[h] = own_b(0, h) + (br[1, 0, h] + br[1, 1, h])
        for i, (_, v, dev) in enumerate(plane[:3]):
            send(bt.at[:, yo(v)], near_b.at[i], dev, ("near_b",), ("near_b",))

    def b_y_sum():
        arrived(near_b, "near_b")
        bf[1] = (bt[ox, y] + near_b[0, ox]) + (near_b[1, ox] + near_b[2, ox])
        send(bf.at[1], bxr, xp, ("bx",), ("bx",))
        bf[0] = (bt[x, y] + near_b[0, x]) + (near_b[1, x] + near_b[2, x])

    def b_final():
        arrived(bxr, "bx")
        gs[:, CA : CA + CB] = bf[0] + bxr[...]

    loads[0].wait()
    y_start(0)
    b_raw4()
    c_raw(0)
    loads[1].wait()
    y_start(1)
    y_direct(0)
    loads[2].wait()
    b_raw3()
    c_raw(1, 2)
    for j in range(3, 8):
        loads[j].wait()
    c_raw(3, 4, 5, 6, 7)
    y_start(2)
    for k in range(8):
        if k + 3 < 7:
            y_start(k + 3)
        for j in ((k,) if k < 2 else (2, 3) if k == 2 else (k + 1,)):
            if j < 7:
                y_forward(j)
        if k + 1 < 7:
            y_direct(k + 1)
        if k == 6:
            near_out(False)
        if k == 0:
            b_forward()
        if k == 1:
            b_two(True)
        if k == 2:
            b_two(False)
        if k == 3:
            b_one(True)
        if k == 4:
            b_one(False)
        if k >= 1:
            y_sum(k - 1)
        if k >= 3:
            z_step(k - 3)
        if k == 1:
            near_out(True)
            c_step(0)
        if k == 2:
            c_step(1, 2)
        if k == 4:
            c_step(3, 4)
        if k == 5:
            b_total()
        if k == 6:
            c_step(5, 6)
    b_y_sum()
    z_step(5)
    c_total()
    z_step(6)
    b_final()
    c_final()
    near_in()

    lane = lax.broadcasted_iota(jnp.int32, (ROWS, 128), 1)
    wide = (ROWS, 1024)
    mine = lax.broadcasted_iota(jnp.int32, wide, 1) == (
        lax.broadcasted_iota(jnp.int32, wide, 0) + me * ROWS
    )
    ids = jnp.sum(jnp.where(mine, in_ref[3, 0:1, 0:1024], 0.0), axis=1, keepdims=True)
    member = (ids == lane.astype(f32)).astype(f32)
    master = in_ref[0]
    mean = gs[...] / 64.0
    new_first = beta_one * in_ref[1] + (1.0 - beta_one) * mean
    new_second = beta_two * in_ref[2] + (1.0 - beta_two) * mean * mean
    own_ref[1] = new_first
    own_ref[2] = new_second
    update = (
        new_first / correct_one / (jnp.sqrt(new_second / correct_two) + adam_eps)
        + weight_decay * master
    )
    gs[...] = update
    weight_rows = jnp.sum(master * master, axis=1, keepdims=True)
    update_rows = jnp.sum(update * update, axis=1, keepdims=True)
    weight_part = jnp.sum(member * weight_rows, axis=0, keepdims=True)
    update_part = jnp.sum(member * update_rows, axis=0, keepdims=True)
    first = lax.broadcasted_iota(jnp.int32, (8, 128), 0) == 0
    norm_send[...] = jnp.where(first, weight_part, update_part)
    for i, p in enumerate(norm_peers):
        send(norm_send, norm_recv.at[i], p, ("norm",), ("norm",))
    arrived(norm_recv, "norm")
    sums = norm_send[...] + jnp.sum(norm_recv[...], axis=0)
    ratio = jnp.sqrt(sums[0:1] / (sums[1:2] + 1e-06))
    row_ratio = jnp.sum(member * ratio, axis=1, keepdims=True)
    step_size = learn_rate * row_ratio * gs[...]
    d[z, x, y] = (-step_size).astype(bf16)

    p_cols = pl.ds(0, PA)
    q_cols = pl.ds(PA, PC)
    halves = (pl.ds(0, 512), pl.ds(512, PA - 512))
    p_units = {1: d.at[0, 0, 0, :, p_cols], 2: d.at[0, :, 0, :, p_cols], 4: d.at[0, 0, :, :, p_cols],
               8: d.at[0, :, :, :, p_cols], 16: d.at[pl.ds(0, 2), :, :, :, p_cols],
               32: d.at[pl.ds(0, 4), :, :, :, p_cols]}
    q_units = {1: d.at[0, 0, 0, :, q_cols], 2: d.at[0, :, 0, :, q_cols], 4: d.at[0, 0, :, :, q_cols],
               8: d.at[0, :, :, :, q_cols], 16: d.at[pl.ds(0, 2), :, :, :, q_cols],
               32: d.at[pl.ds(0, 4), :, :, :, q_cols]}
    spans = (32, 16, 8, 4, 2, 1)
    count = {"p": 0, "q": 0}

    def hop(kind, ref, dev, *into, whole=True):
        group = next(i for i in range(6) if count[kind] < sum(spans[: i + 1]))
        send(ref, ref, dev, (kind, group), into)
        count[kind] += whole

    def z_own():
        ref = d.at[z, x, y, :, p_cols]
        for step, up, down in ((1, zu, zd), (2, zu2, zd2)):
            hop("p", ref, up, "az", step)
            hop("p", ref, down, "az", step)

    def y_out(other, *dzs):
        h = ox if other else x
        for dz in dzs:
            ref = d.at[zo(dz), h, y, :, p_cols]
            far = (dz, other) in FAR
            relayed = ("relay", abs(dz), other)
            hop("p", ref, yu, *(("end", dz) if far or other else relayed))
            hop("p", ref, yd, *(("end", dz) if far or not other else relayed))
            if far:
                hop("p", ref, y2, "far", dz)

    def x_out(*dzs):
        for dz in dzs:
            hop("p", d.at[zo(dz), x, y, :, p_cols], xp, "ax", abs(dz))

    def x_in(*dzs):
        arrived(p_units[len(dzs)], "ax", abs(dzs[0]))
        y_out(True, *dzs)

    def y_relay(other, *dzs):
        arrived(p_units[len(dzs)], "relay", abs(dzs[0]), other)
        for dz in dzs:
            if other:
                hop("p", d.at[zo(dz), ox, yo(1), :, p_cols], yd, "end", dz)
            else:
                hop("p", d.at[zo(dz), x, yo(-1), :, p_cols], yu, "end", dz)

    def z_in(step):
        arrived(p_units[1 if step == 4 else 2], "az", step)
        if step == 2:
            hop("p", d.at[zo(-2), x, y, :, p_cols], zu, "az", 3)
            hop("p", d.at[zo(2), x, y, :, p_cols], zd, "az", 3)
            hop("p", d.at[zo(-2), x, y, :, halves[0]], zu2, "az", 4, whole=False)
            hop("p", d.at[zo(2), x, y, :, halves[1]], zd2, "az", 4)
        dzs = (-step, step) if step < 4 else (4,)
        x_out(*dzs)
        y_out(False, *dzs)

    def q_out(step, other, v):
        h = ox if other else x
        far = step - 1
        for s, dev in ((0, zu), (1, zd)):
            if step == 4 and s != int(other):
                continue
            if step == 4:
                into = ("q4",)
            elif step == 3 and s != int(other):
                into = ("q3", 3 if s else -3)
            else:
                into = ("q", step, other, v)
            hop("q", d.at[zo(-far if s == 0 else far), h, yo(v), :, q_cols], dev, *into)

    def q_in(step, other, *vs):
        for v in vs:
            arrived(q_units[1 if step == 3 else 2], "q", step, other, v)
            q_out(step + 1, other, v)

    def plane_out():
        for other, v, dev in plane:
            hop("q", d.at[z, x, y, :, q_cols], dev, "plane", other, v if v == 2 else -v)

    def plane_in(other, *vs):
        for v in vs:
            arrived(q_units[1], "plane", other, v)
            q_out(1, other, v)

    def slab_out(*dzs):
        for dz in dzs:
            arrived(p_units[4], "end", dz)
            if dz in (0, 4):
                arrived(p_units[1], "far", dz)
            if abs(dz) == 3:
                arrived(q_units[4], "q3", dz)
            if dz == 4:
                arrived(q_units[8], "q4")
            zz = zo(dz)

            def add(i, _):
                h, v = lax.div(i, NY), lax.rem(i, NY)
                nw_ref[zz, h, v] = (w[zz, h, v].astype(f32) + d[zz, h, v].astype(f32)).astype(bf16)
                return 0

            lax.fori_loop(0, NX * NY, add, 0)

    q_out(1, False, 0)
    plane_out()
    z_own()
    y_out(False, 0)
    x_out(0)
    own_ref[0] = in_ref[0] - step_size
    q_in(1, False, 0)
    z_in(1)
    plane_in(False, 1, -1)
    plane_in(True, 0)
    z_in(2)
    x_in(0)
    plane_in(False, 2)
    plane_in(True, 1, -1, 2)
    q_in(2, False, 0)
    y_relay(False, -1, 1)
    q_in(1, False, 1, -1)
    z_in(3)
    q_in(1, True, 0)
    x_in(-1, 1)
    q_in(1, False, 2)
    z_in(4)
    q_in(1, True, 1, -1, 2)
    y_relay(False, -2, 2)
    x_in(-2, 2)
    y_relay(True, 0)
    q_in(3, False, 0)
    q_in(2, False, 1, -1)
    q_in(2, True, 0)
    x_in(-3, 3)
    y_relay(False, -3, 3)
    q_in(2, False, 2)
    y_relay(True, -1, 1)
    x_in(4)
    q_in(2, True, 1, -1, 2)
    y_relay(True, -2, 2)
    y_relay(False, 4)
    q_in(3, False, 1, -1)
    q_in(3, True, 0)
    y_relay(True, -3, 3)
    q_in(3, False, 2)
    loads[8].wait()
    slab_out(0, -1, 1)
    q_in(3, True, 1, -1, 2)
    gone(g.at[pl.ds(0, 7), :, :, :, a_cols], "y")
    gone(xs, "x")
    gone(zs, "z")
    gone(g.at[pl.ds(0, 4), :, :, :, b_cols], "b")
    gone(bs, "bs")
    gone(near_a, "near_a")
    gone(near_b, "near_b")
    gone(bxr, "bx")
    gone(cx, "cx")
    gone(cs, "cz")
    gone(cn, "cn")
    gone(norm_recv, "norm")
    slab_out(-2, 2)
    slab_out(-3, 3)
    slab_out(4)
    for i, n in enumerate(spans):
        gone(p_units[n], "p", i)
        gone(q_units[n], "q", i)
    assert count == {"p": 63, "q": 63}
    assert (len(send_ids), len(recv_ids)) == (N_SEND, N_RECV), (len(send_ids), len(recv_ids))


def write_out(nw_ref, own_ref, nw_hbm, nm_hbm, nf_hbm, ns_hbm, sem):
    copies = []
    for i in range(4):
        rows = pl.ds(256 * i, 256)
        copies.append(pltpu.make_async_copy(nw_ref.at[rows], nw_hbm.at[rows], sem.at[i]))
    for i, to in enumerate((nm_hbm, nf_hbm, ns_hbm)):
        copies.append(pltpu.make_async_copy(own_ref.at[i], to, sem.at[4 + i]))
    for c in copies:
        c.start()
    for c in copies:
        c.wait()


def on_device(gradients, weights, master, moment_one, moment_two, group_ids):
    V = pltpu.VMEM
    scratch = [
        V((NZ, NX, NY, ROWS, COLS), bf16),
        V((NZ, NX, NY, ROWS, COLS), bf16),
        V((NZ, NX, NY, ROWS, COLS), bf16),
        V((7, 6, ROWS, CA), bf16),
        V((7, 2, ROWS, CA), bf16),
        V((7, ROWS, CA), f32),
        V((7, ROWS, CA), f32),
        V((7, ROWS, CA), f32),
        V((7, ROWS, CA), f32),
        V((7, ROWS, CA), f32),
        V((2, NY, ROWS, CB), bf16),
        V((2, NY, ROWS, CB), bf16),
        V((2, 2, NY, ROWS, CB), bf16),
        V((2, 2, 2, NY, ROWS, CB), f32),
        V((2, 2, 2, NY, ROWS, CB), f32),
        V((2, NY, ROWS, CB), f32),
        V((7, ROWS, CA), bf16),
        V((3, 2, ROWS, CB), f32),
        V((2, ROWS, CB), f32),
        V((ROWS, CB), f32),
        V((8, NY, ROWS, CC), bf16),
        V((7, NY, ROWS, CC), f32),
        V((7, NY, ROWS, CC), f32),
        V((NY, ROWS, CC), f32),
        V((3, ROWS, CC), f32),
        V((ROWS, COLS), f32),
        V((8, 128), f32),
        V((35, 8, 128), f32),
        pltpu.SemaphoreType.DMA((9,)),
        pltpu.SemaphoreType.DMA((N_SEND,)),
        pltpu.SemaphoreType.DMA((N_RECV,)),
    ]
    hbm, vmem = pl.BlockSpec(memory_space=pltpu.HBM), pl.BlockSpec(memory_space=pltpu.VMEM)
    ids = jnp.pad(group_ids.astype(f32).reshape(1, 1024), ((0, ROWS - 1), (0, COLS - 1024)))
    inputs = jnp.stack([master, moment_one, moment_two, ids])
    new_weights, own = pl.pallas_call(
        kernel,
        out_shape=(
            jax.ShapeDtypeStruct((NZ, NX, NY, ROWS, COLS), bf16),
            jax.ShapeDtypeStruct((3, ROWS, COLS), f32),
        ),
        in_specs=[hbm, hbm, vmem],
        out_specs=(vmem, vmem),
        scratch_shapes=scratch,
        name="lamb",
        compiler_params=pltpu.CompilerParams(
            collective_id=0, has_side_effects=True, vmem_limit_bytes=48 * 2**20
        ),
    )(
        gradients.reshape(NZ, NX, NY, ROWS, COLS),
        weights.reshape(NZ, NX, NY, ROWS, COLS),
        inputs,
    )
    row_block = jax.ShapeDtypeStruct((ROWS, COLS), f32)
    new_weights, new_master, new_first, new_second = pl.pallas_call(
        write_out,
        out_shape=(jax.ShapeDtypeStruct((1024, COLS), bf16),) + (row_block,) * 3,
        in_specs=[pl.BlockSpec(memory_space=pl.ANY)] * 2,
        out_specs=(hbm,) * 4,
        scratch_shapes=[pltpu.SemaphoreType.DMA((7,))],
        compiler_params=pltpu.CompilerParams(vmem_limit_bytes=2**20),
        name="out",
    )(new_weights.reshape(1024, COLS), own)
    return (new_weights, new_master, new_first, new_second)


def solution(mesh):
    torus = Mesh(mesh.devices.reshape(8, 2, 4, 2, 2), NAMES)
    dp, mp = ("z", "xh", "y"), ("xl", "c")
    return jax.shard_map(
        on_device,
        mesh=torus,
        in_specs=(P(dp, None, mp), P(None, mp), P(dp, mp), P(dp, mp), P(dp, mp), P()),
        out_specs=(P(None, mp), P(dp, mp), P(dp, mp), P(dp, mp)),
        check_vma=False,
    )
```
